32 devices in a mesh: prow: 4 (over x, core), pcol: 8 (over z, y).
Axes of the slice: x: 2, y: 2, z: 4, core: 2. Of those that a mesh axis runs over, the one named last changes fastest.
Arguments:
- child_u: bfloat16 [2, 10, 4, 2, 8, 512, 128], P(None, None, 'prow', None, 'pcol'), may hold values from -5 to 5
- child_v: bfloat16 [2, 10, 4, 2, 8, 512, 128], P(None, None, 'prow', None, 'pcol'), may hold values from -5 to 5
- child_rank: int32 [2, 10, 4, 2, 8], P(None, None, 'prow', None, 'pcol'), may hold values from 0 to 128, as said below
- diag_shift: float32 [16, 512], replicated, may hold values from 0.5 to 4
Outputs:
- front_out: float32 [10, 4, 512, 2, 8, 512], P(None, 'prow', None, None, 'pcol')
The draws below stay inside these ranges and needn't reach their ends.
Inputs may be any that keep to these rules, and one draw needn't show every extreme that they name: `child_rank`: 0 on and above the block diagonal (i <= j); below it 0 where the child has no tile, else from 16 to 128.
All inputs are finite; a program needn't handle non-finite values.
Results may differ from the reference program's by a relative error of at most 0.0003.
Values may be sent and summed in bfloat16 or wider, within the bound.
A program may use at most 320 MiB of HBM per device.

```python
import math
import jax
import jax.numpy as jnp
from jax import lax

BLOCK = 512
RANK_MAX = 128
CHILDREN = 2
PANELS = 2
NBLK = 40
SLAB = 16
N_PROW = 4
N_PCOL = 8


def draw_child_rank(key, part):
    key_rank = jax.random.fold_in(key, 11)
    key_keep = jax.random.fold_in(key, 23)
    shape = (CHILDREN, NBLK // N_PROW, N_PROW, SLAB // N_PCOL, N_PCOL)
    block_rows = lax.broadcasted_iota(jnp.int32, shape, 1) * N_PROW + lax.broadcasted_iota(jnp.int32, shape, 2)
    block_cols = lax.broadcasted_iota(jnp.int32, shape, 3) * N_PCOL + lax.broadcasted_iota(jnp.int32, shape, 4)
    ranks = jax.random.randint(key_rank, shape, RANK_MAX // 8, RANK_MAX + 1)
    present = jax.random.randint(key_keep, shape, 0, 4) > 0
    return jnp.where((block_rows > block_cols) & present, ranks, 0).astype(jnp.int32)


def block_levels(key, dims, split, smallest, top_value):
    loudness, own = 1.0, jax.random.fold_in(key, 6)
    for position, blocks in split:
        steps = jnp.exp(jax.random.uniform(jax.random.fold_in(own, position), (blocks,), jnp.float32, smallest / len(split), top_value / len(split)))
        loudness = loudness * jnp.repeat(steps, dims[position] // blocks).reshape([-1 if axis == position else 1 for axis in range(len(dims))])
    return loudness


def scatter_about(key, shape, deviation, limit, pieces=(), kind=jnp.bfloat16):
    array = deviation * jax.random.normal(key, shape, jnp.float32)
    if pieces:
        array = array * block_levels(key, shape, pieces, -0.22, 0.18)
    return jnp.clip(array, -limit, limit).astype(kind)


def setup_inputs(seed: int = 0) -> dict:
    splits = jax.random.split(jax.random.key(seed), 5)
    child_u = scatter_about(splits[0], (CHILDREN, NBLK // N_PROW, N_PROW, SLAB // N_PCOL, N_PCOL, BLOCK, RANK_MAX), 0.35, 5.0, ((2, 4), (4, 8)))
    child_v = scatter_about(splits[1], (CHILDREN, NBLK // N_PROW, N_PROW, SLAB // N_PCOL, N_PCOL, BLOCK, RANK_MAX), 0.35, 5.0, ((2, 4), (4, 8)))
    child_rank = draw_child_rank(jax.random.fold_in(splits[4], 71), 0)
    diag_shift = jnp.clip(jnp.exp(jax.random.uniform(splits[3], (SLAB, BLOCK), jnp.float32, math.log(0.5), math.log(4.0))), 0.5, 4.0)
    return {"child_u": child_u, "child_v": child_v, "child_rank": child_rank, "diag_shift": diag_shift}


def reference(child_u, child_v, child_rank, diag_shift):
    precise = lax.Precision.HIGHEST
    rank_grid = child_rank.reshape(CHILDREN, NBLK, SLAB)
    keep_mask = (jnp.arange(RANK_MAX, dtype=jnp.int32)[None, None, None, :] < rank_grid[:, :, :, None]).astype(jnp.bfloat16)
    left_factor = child_u.reshape(CHILDREN, NBLK, SLAB, BLOCK, RANK_MAX) * keep_mask[:, :, :, None, :]
    right_factor = child_v.reshape(CHILDREN, NBLK, SLAB, BLOCK, RANK_MAX) * keep_mask[:, :, :, None, :]
    left_cols = left_factor.transpose(2, 0, 1, 3, 4)
    right_cols = right_factor.transpose(2, 0, 1, 3, 4)

    def assemble(operands):
        left_part = operands[0].astype(jnp.float32)
        right_part = operands[1].astype(jnp.float32)
        tile_col = jnp.einsum('ciak,cibk->iab', left_part, right_part, precision=precise)
        column_sum = jnp.einsum('ciak,cibk->ab', right_part, right_part, precision=precise)
        return (tile_col, column_sum)
    front_cols, column_sums = lax.map(assemble, (left_cols, right_cols))

    def row_part(row_factor):
        row_factor = row_factor.astype(jnp.float32)
        return jnp.einsum('cjak,cjbk->ab', row_factor, row_factor, precision=precise)
    row_sums = lax.map(row_part, left_factor.transpose(1, 0, 2, 3, 4)[:SLAB])
    diagonal_index = jnp.arange(SLAB, dtype=jnp.int32)
    identity = jnp.eye(BLOCK, dtype=jnp.float32)
    diag_terms = row_sums + column_sums + identity[None] * diag_shift[:, None, :]
    front_cols = front_cols.at[diagonal_index, diagonal_index].add(diag_terms)
    block_rows = jnp.arange(NBLK, dtype=jnp.int32)
    panel_list = []
    for panel_index in range(PANELS):
        factor = jnp.linalg.cholesky(front_cols[panel_index, panel_index])
        solved = lax.linalg.triangular_solve(factor, front_cols[panel_index].reshape(NBLK * BLOCK, BLOCK), left_side=False, lower=True, transpose_a=True).reshape(NBLK, BLOCK, BLOCK)
        below_mask = (block_rows > panel_index)[:, None, None]
        solved = jnp.where(below_mask, solved, 0.0)
        pivot_diag = jnp.diagonal(factor)
        at_pivot = (block_rows == panel_index)[:, None, None]
        panel_list.append(jnp.where(at_pivot, (factor * pivot_diag[None, :])[None], solved * pivot_diag[None, None, :]))
        rounded = lax.optimization_barrier(solved.astype(jnp.bfloat16)).astype(jnp.float32)

        def update(operands, rounded=rounded):
            return operands[0] - jnp.einsum('iab,cb->iac', rounded, operands[1], precision=precise)
        front_cols = lax.map(update, (front_cols, rounded[:SLAB]))
    slab_index = jnp.arange(SLAB, dtype=jnp.int32)
    lower_mask = (block_rows[None, :] >= slab_index[:, None])[:, :, None, None]
    final = jnp.where(lower_mask, front_cols, 0.0)
    final = final.at[:PANELS].set(jnp.stack(panel_list))
    final = final.reshape(SLAB // N_PCOL, N_PCOL, NBLK // N_PROW, N_PROW, BLOCK, BLOCK).transpose(2, 3, 4, 0, 1, 5)
    return final
```

```python
import functools

import jax
import jax.numpy as jnp
from jax import lax
from jax.experimental import pallas as pl
from jax.experimental.pallas import tpu as pltpu
from jax.sharding import PartitionSpec as P

PANELS = 2
STEP = 128
SUB = 8
PAIRS = [(m, k) for k in range(PANELS) for m in range(k + 1, PANELS)]
MESH = pl.DeviceIdType.MESH
ANY = pl.BlockSpec(memory_space=pl.ANY)


def nt(a, b, precision=None):
    return lax.dot_general(
        a, b, (((1,), (1,)), ((), ())), preferred_element_type=jnp.float32, precision=precision
    )


def nn(a, b, precision=None):
    return lax.dot_general(
        a, b, (((1,), (0,)), ((), ())), preferred_element_type=jnp.float32, precision=precision
    )


def split(value):
    high = value.astype(jnp.bfloat16)
    low = (value - high.astype(jnp.float32)).astype(jnp.bfloat16)
    return high, low


def prep_kernel(dims, at_ref, rank_ref, u_ref, v_ref, pan_ref, sum_ref, row_ref):
    prow, pcol, kept, tiles = dims
    r = pl.program_id(0)
    children, cols = u_ref.shape[0], u_ref.shape[3]
    rank_max = u_ref.shape[-1]
    lane = lax.broadcasted_iota(jnp.int32, (1, rank_max), 1)

    @pl.when(r == 0)
    def _():
        sum_ref[...] = jnp.zeros_like(sum_ref)

    for t in range(cols):
        left, right = [], []
        for c in range(children):
            rank = rank_ref[(c * pl.num_programs(0) + r) * cols + t]
            keep = (lane < rank).astype(jnp.bfloat16)
            left.append(u_ref[c, 0, 0, t, 0] * keep)
            right.append(v_ref[c, 0, 0, t, 0] * keep)
        if t == 0:
            for c in range(children):
                pan_ref[0, 0, 0, c] = left[c]
                pan_ref[0, 0, 1, c] = right[c]
        if t < tiles:

            @pl.when(r < kept)
            def _(left=left, t=t):
                for c in range(children):
                    row_ref[0, t, c] = left[c]

        wide = jnp.concatenate(right, axis=1)
        sum_ref[t] += nt(wide, wide)
        i = r * prow + at_ref[0]
        j = t * pcol + at_ref[1]

        @pl.when((i == j) & (j < PANELS))
        def _(left=left, wide=wide, t=t):
            sum_ref[t] += nt(jnp.concatenate(left, axis=1), wide)


def prep(prow, pcol, kept, tiles, at, ranks, child_u, child_v):
    children, rows, _, cols, _, extent, rank = child_u.shape
    tile = pl.BlockSpec(
        (children, 1, 1, cols, 1, extent, rank), lambda r, at, ranks: (0, r, 0, 0, 0, 0, 0)
    )
    return pl.pallas_call(
        functools.partial(prep_kernel, (prow, pcol, kept, tiles)),
        out_shape=(
            jax.ShapeDtypeStruct((PANELS, rows, 2, children, extent, rank), jnp.bfloat16),
            jax.ShapeDtypeStruct((cols, extent, extent), jnp.float32),
            jax.ShapeDtypeStruct((kept, tiles, children, extent, rank), jnp.bfloat16),
        ),
        grid_spec=pltpu.PrefetchScalarGridSpec(
            num_scalar_prefetch=2,
            grid=(rows,),
            in_specs=[tile, tile],
            out_specs=(
                pl.BlockSpec(
                    (1, 1, 2, children, extent, rank),
                    lambda r, at, ranks: (lax.rem(at[1], PANELS), r, 0, 0, 0, 0),
                ),
                pl.BlockSpec((cols, extent, extent), lambda r, at, ranks: (0, 0, 0)),
                pl.BlockSpec(
                    (1, tiles, children, extent, rank),
                    lambda r, at, ranks: (jnp.minimum(r, kept - 1), 0, 0, 0, 0),
                ),
            ),
        ),
        compiler_params=pltpu.CompilerParams(vmem_limit_bytes=40 * 2**20),
        cost_estimate=pl.CostEstimate(
            flops=2 * rows * cols * extent * extent * children * rank,
            bytes_accessed=18 * 2**20,
            transcendentals=0,
        ),
        name="prep",
    )(at, ranks, child_u, child_v)


def exchange_kernel(dims, pan_in, sum_ref, row_ref, pan, oth, rowbuf, sumbuf, piv, pair, *scratch):
    prow, pcol, rows, cols, kept, tiles = dims
    (part, total, bounce, local, part_s, part_r, sum_s, sum_r, row_s, row_r, chain_s, chain_r,
     cross_s, cross_r, oth_s, oth_r, pair_s, pair_r, gat_s, gat_r) = scratch
    del pan_in
    p, q = lax.axis_index("prow"), lax.axis_index("pcol")
    z, y = q // PANELS, lax.rem(q, PANELS)
    depth = pcol // PANELS
    home = lax.rem(q, prow)
    extent = sum_ref.shape[-1]
    band = extent // prow

    barrier = pltpu.get_barrier_semaphore()
    for d in range(1, pcol):
        pl.semaphore_signal(
            barrier, inc=1, device_id={"pcol": lax.rem(q + d, pcol)}, device_id_type=MESH
        )
    for d in range(1, prow):
        pl.semaphore_signal(
            barrier, inc=1, device_id={"prow": lax.rem(p + d, prow)}, device_id_type=MESH
        )
    pl.semaphore_wait(barrier, pcol + prow - 2)

    def send(src, dst, send_sem, recv_sem, **target):
        return pltpu.make_async_remote_copy(
            src_ref=src, dst_ref=dst, send_sem=send_sem, recv_sem=recv_sem,
            device_id=target, device_id_type=MESH,
        )

    def part_copy(d):
        s = lax.rem(p + d, prow)
        return send(
            sum_ref.at[0, pl.ds(pl.multiple_of(s * band, 8), band)], part.at[d],
            part_s.at[d - 1], part_r.at[d - 1], prow=s,
        )

    def sum_copy():
        d = lax.rem(home + prow - p, prow) - 1
        return send(sum_ref, sumbuf.at[d], sum_s, sum_r.at[d], prow=home)

    def sum_arrival(d):
        return send(sum_ref, sumbuf.at[d], sum_s, sum_r.at[d], prow=home)

    def reach(r):
        return sum(1 for t in range(tiles) if t * pcol < (r + 1) * prow)

    def row_copy(r, first):
        i = r * prow + p
        owner, slot = lax.rem(i, pcol), i // pcol
        window = pl.ds(first, reach(r) - first)
        return send(
            row_ref.at[r, window], rowbuf.at[slot, q, window], row_s.at[r], row_r.at[slot, q],
            pcol=owner,
        )

    def row_arrival(slot, origin, r, first):
        window = pl.ds(first, reach(r) - first)
        return send(
            row_ref.at[r, window], rowbuf.at[slot, origin, window], row_s.at[r],
            row_r.at[slot, origin], pcol=origin,
        )

    def chain_copy(n):
        ref = pan.at[y, n // 2, n % 2] if n < 2 * rows else piv.at[y, p]
        return send(ref, ref, chain_s.at[n], chain_r.at[n], pcol=q + PANELS)

    def cross_copy(n, which):
        ref = pan.at[which, n // 2, n % 2] if n < 2 * rows else piv.at[which, p]
        return send(ref, ref, cross_s.at[n], cross_r.at[n], pcol=q + 1 - 2 * y)

    def forward(n):
        @pl.when(z < depth - 1)
        def _():
            chain_copy(n).start()

        cross_copy(n, y).start()

    def oth_row(t):
        return (t * pcol + q) // prow

    def oth_copy(t, k, d):
        n = t * PANELS + k
        return send(
            pan.at[k, oth_row(t)], oth.at[t, k], oth_s.at[n, d - 1], oth_r.at[n],
            prow=lax.rem(p + d, prow),
        )

    def pair_copy(n, d):
        m, k = PAIRS[n]
        return send(
            pan.at[k, m // prow], pair.at[n], pair_s.at[n, d - 1], pair_r.at[n],
            prow=lax.rem(p + d, prow),
        )

    def gat_copy(k, d):
        return send(
            piv.at[k, p], piv.at[k, p], gat_s.at[k, d - 1], gat_r.at[k, d - 1],
            prow=lax.rem(p + d, prow),
        )

    def gat_arrival(k, d):
        o = lax.rem(p + prow - d, prow)
        return send(
            piv.at[k, o], piv.at[k, o], gat_s.at[k, d - 1], gat_r.at[k, d - 1], prow=o
        )

    @pl.when(z == 0)
    def _():
        for d in range(1, prow):
            part_copy(d).start()
        pltpu.make_async_copy(
            sum_ref.at[0, pl.ds(pl.multiple_of(p * band, 8), band)], part.at[0], local.at[0]
        ).start()

    @pl.when(p != home)
    def _():
        sum_copy().start()

    for r in range(kept):
        owner = lax.rem(r * prow + p, pcol)

        @pl.when((q != owner) & (z > 0))
        def _():
            row_copy(r, 0).start()

        if reach(r) > 1:

            @pl.when((q != owner) & (z == 0))
            def _():
                row_copy(r, 1).start()

    last = 2 * rows

    def step(n):
        @pl.when(z > 0)
        def _():
            chain_copy(n).wait_recv()

        forward(n)

    step(0)
    step(1)

    @pl.when(z == 0)
    def _():
        pltpu.make_async_copy(
            sum_ref.at[0, pl.ds(pl.multiple_of(p * band, 8), band)], part.at[0], local.at[0]
        ).wait()
        for d in range(1, prow):
            part_copy(d).wait_recv()
        value = part[0]
        for d in range(1, prow):
            value = value + part[d]
        total[...] = value
        out = pltpu.make_async_copy(total, piv.at[y, p], local.at[1])
        out.start()
        out.wait()

    step(last)
    near = 2 * kept
    for n in range(2, near + 2):
        step(n)

    cross_copy(last, 1 - y).wait_recv()
    for n in range(near):
        cross_copy(n, 1 - y).wait_recv()

    for k in range(PANELS):
        for d in range(1, prow):
            gat_copy(k, d).start()
    for n, (m, k) in enumerate(PAIRS):

        @pl.when(p == m % prow)
        def _():
            for d in range(1, prow):
                pair_copy(n, d).start()
            slot = cols * PANELS + n
            load = pltpu.make_async_copy(pan.at[k, m // prow], bounce.at[slot], local.at[2 + slot])
            load.start()
            load.wait()
            store = pltpu.make_async_copy(bounce.at[slot], pair.at[n], local.at[2 + slot])
            store.start()
            store.wait()

    @pl.when(p == home)
    def _():
        for t in range(cols):
            for k in range(PANELS):
                for d in range(1, prow):
                    oth_copy(t, k, d).start()
        loads = [
            pltpu.make_async_copy(
                pan.at[k, oth_row(t)], bounce.at[t * PANELS + k], local.at[2 + t * PANELS + k]
            )
            for t in range(cols)
            for k in range(PANELS)
        ]
        stores = [
            pltpu.make_async_copy(
                bounce.at[t * PANELS + k], oth.at[t, k], local.at[2 + t * PANELS + k]
            )
            for t in range(cols)
            for k in range(PANELS)
        ]
        for load in loads:
            load.start()
        for load, store in zip(loads, stores):
            load.wait()
            store.start()
        for store in stores:
            store.wait()

    for n in range(near + 2, last):
        step(n)
    for n in range(near, last):
        cross_copy(n, 1 - y).wait_recv()

    for k in range(PANELS):
        for d in range(1, prow):
            gat_arrival(k, d).wait_recv()
            gat_copy(k, d).wait_send()
    for n, (m, k) in enumerate(PAIRS):

        @pl.when(p == m % prow)
        def _():
            for d in range(1, prow):
                pair_copy(n, d).wait_send()

        @pl.when(p != m % prow)
        def _():
            pair_copy(n, 1).wait_recv()

    @pl.when(p == home)
    def _():
        for t in range(cols):
            for k in range(PANELS):
                for d in range(1, prow):
                    oth_copy(t, k, d).wait_send()
        for d in range(prow - 1):
            sum_arrival(d).wait_recv()
        for slot in range(cols):
            for origin in range(pcol):

                @pl.when(q != origin)
                def _():
                    low = slot * pcol // prow
                    first = 1 if origin < PANELS else 0
                    if reach(low) > first:
                        row_arrival(slot, origin, low, first).wait_recv()

    @pl.when(p != home)
    def _():
        for t in range(cols):
            for k in range(PANELS):
                oth_copy(t, k, 1).wait_recv()
        sum_copy().wait_send()

    @pl.when(z == 0)
    def _():
        for d in range(1, prow):
            part_copy(d).wait_send()

    for r in range(kept):
        owner = lax.rem(r * prow + p, pcol)

        @pl.when((q != owner) & (z > 0))
        def _():
            row_copy(r, 0).wait_send()

        if reach(r) > 1:

            @pl.when((q != owner) & (z == 0))
            def _():
                row_copy(r, 1).wait_send()

    for n in range(last + 1):

        @pl.when(z < depth - 1)
        def _():
            chain_copy(n).wait_send()

        cross_copy(n, y).wait_send()


def exchange(prow, pcol, pan, sums, rowtiles):
    _, rows, _, children, extent, rank = pan.shape
    cols = sums.shape[0]
    kept, tiles = rowtiles.shape[:2]
    band = extent // prow
    pairs = max(len(PAIRS), 1)
    dma = pltpu.SemaphoreType.DMA
    return pl.pallas_call(
        functools.partial(exchange_kernel, (prow, pcol, rows, cols, kept, tiles)),
        out_shape=(
            jax.ShapeDtypeStruct(pan.shape, pan.dtype),
            jax.ShapeDtypeStruct((cols, PANELS, 2, children, extent, rank), pan.dtype),
            jax.ShapeDtypeStruct((cols, pcol, tiles, children, extent, rank), pan.dtype),
            jax.ShapeDtypeStruct((prow - 1, cols, extent, extent), jnp.float32),
            jax.ShapeDtypeStruct((PANELS, prow, band, extent), jnp.float32),
            jax.ShapeDtypeStruct((pairs, 2, children, extent, rank), pan.dtype),
        ),
        in_specs=[ANY, ANY, ANY],
        out_specs=(ANY,) * 6,
        scratch_shapes=[
            pltpu.VMEM((prow, band, extent), jnp.float32),
            pltpu.VMEM((band, extent), jnp.float32),
            pltpu.VMEM((cols * PANELS + pairs, 2, children, extent, rank), pan.dtype),
            dma((2 + cols * PANELS + pairs,)),
            dma((prow - 1,)),
            dma((prow - 1,)),
            dma,
            dma((prow - 1,)),
            dma((kept,)),
            dma((cols, pcol)),
            dma((2 * rows + 1,)),
            dma((2 * rows + 1,)),
            dma((2 * rows + 1,)),
            dma((2 * rows + 1,)),
            dma((cols * PANELS, prow - 1)),
            dma((cols * PANELS,)),
            dma((pairs, prow - 1)),
            dma((pairs,)),
            dma((PANELS, prow - 1)),
            dma((PANELS, prow - 1)),
        ],
        input_output_aliases={0: 0},
        compiler_params=pltpu.CompilerParams(
            collective_id=0, has_side_effects=True, vmem_limit_bytes=40 * 2**20
        ),
        cost_estimate=pl.CostEstimate(
            flops=120_000_000_000, bytes_accessed=60 * 2**20, transcendentals=0
        ),
        name="exchange",
    )(pan, sums, rowtiles)


def factor_step(w_ref, e_ref, c_ref, y_ref):
    extent = w_ref.shape[0]
    exact = lax.Precision.HIGHEST
    groups = STEP // SUB
    sub_row = lax.broadcasted_iota(jnp.int32, (SUB, STEP), 0)
    lane = lax.broadcasted_iota(jnp.int32, (SUB, STEP), 1)

    @pl.loop(0, extent // STEP)
    def _(block):
        base = pl.multiple_of(block * STEP, STEP)
        here = pl.ds(base, STEP)
        tile = w_ref[here, here]
        left = [tile[g * SUB : (g + 1) * SUB] for g in range(groups)]
        right = [(lane == sub_row + g * SUB).astype(jnp.float32) for g in range(groups)]
        for j in range(STEP):
            own, inner = divmod(j, SUB)
            row = left[own][inner : inner + 1]
            inverse = 1.0 / jnp.broadcast_to(row[:, j : j + 1], (1, STEP))
            row_left = jnp.broadcast_to(row * inverse, (SUB, STEP))
            row_right = jnp.broadcast_to(right[own][inner : inner + 1] * inverse, (SUB, STEP))
            for g in range(own, groups):
                weight = jnp.broadcast_to(left[g][:, j : j + 1], (SUB, STEP))
                if g == own:
                    weight = jnp.where(sub_row > inner, weight, 0.0)
                left[g] = left[g] - weight * row_left
                right[g] = right[g] - weight * row_right
        upper = jnp.concatenate(left, axis=0)
        lower_inverse = jnp.concatenate(right, axis=0)
        tile_row = lax.broadcasted_iota(jnp.int32, (STEP, STEP), 0)
        tile_col = lax.broadcasted_iota(jnp.int32, (STEP, STEP), 1)
        pivots = jnp.sum(jnp.where(tile_row == tile_col, upper, 0.0), axis=1, keepdims=True)
        root = jnp.sqrt(pivots)
        pivot_factor = (jnp.where(tile_row <= tile_col, upper, 0.0) / root).T
        pivot_inverse = lower_inverse / root
        panel = nt(w_ref[:, here], pivot_inverse, exact)
        below = lax.broadcasted_iota(jnp.int32, (extent, STEP), 0) >= base + STEP
        panel = jnp.where(below, panel, 0.0)
        c_ref[:, here] = panel
        c_ref[here, here] = pivot_factor
        solved = nn(pivot_inverse, e_ref[here, :], exact)
        y_ref[here, :] = solved
        w_ref[...] -= nt(panel, panel, exact)
        e_ref[...] -= nn(panel, solved, exact)


def pivot_kernel(piv_ref, shift_ref, pair_ref, c_ref, inv_ref, car_ref, w_ref, e_ref, y_ref, g_ref):
    extent = w_ref.shape[0]
    children = pair_ref.shape[2]
    eye = lax.broadcasted_iota(jnp.int32, (extent, extent), 0) == lax.broadcasted_iota(
        jnp.int32, (extent, extent), 1
    )

    def wide(n, side):
        return jnp.concatenate([pair_ref[n, side, c] for c in range(children)], axis=1)

    @pl.loop(0, PANELS)
    def _(k):
        w_ref[...] = piv_ref[k] + jnp.where(eye, shift_ref[k], 0.0)
        for n, (m, _) in enumerate(PAIRS):

            @pl.when(k == m)
            def _():
                left = wide(n, 0)
                g = g_ref[n]
                w_ref[...] += nt(left, left) - nt(g, g)

        e_ref[...] = eye.astype(jnp.float32)
        factor_step(w_ref, e_ref, c_ref.at[k], y_ref)
        high, low = split(y_ref[...])
        inv_ref[k, 0] = high
        inv_ref[k, 1] = low

        for n, (m, kk) in enumerate(PAIRS):

            @pl.when(k == kk)
            def _():
                right = wide(n, 1)
                moved = split(nn(high, right) + nn(low, right))
                left = wide(n, 0)
                value = nt(left, moved[0]) + nt(left, moved[1])
                for o, (mo, ko) in enumerate(PAIRS):
                    if mo == m and ko < kk:
                        carry = [car_ref[PAIRS.index((kk, ko)), s] for s in range(2)]
                        value = value - nt(g_ref[o], carry[0]) - nt(g_ref[o], carry[1])
                g_ref[n] = value.astype(jnp.bfloat16)

            @pl.when(k == m)
            def _():
                g = g_ref[n]
                one, two = split(nn(high, g) + nn(low, g))
                car_ref[n, 0] = one
                car_ref[n, 1] = two


def pivots(piv, shift, pair):
    extent = piv.shape[-1]
    pairs = pair.shape[0]
    spec = pl.BlockSpec(memory_space=pltpu.VMEM)
    square = (extent, extent)
    return pl.pallas_call(
        pivot_kernel,
        out_shape=(
            jax.ShapeDtypeStruct((PANELS,) + square, jnp.float32),
            jax.ShapeDtypeStruct((PANELS, 2) + square, jnp.bfloat16),
            jax.ShapeDtypeStruct((pairs, 2) + square, jnp.bfloat16),
        ),
        in_specs=[spec] * 3,
        out_specs=(spec,) * 3,
        scratch_shapes=[
            pltpu.VMEM(square, jnp.float32),
            pltpu.VMEM(square, jnp.float32),
            pltpu.VMEM(square, jnp.float32),
            pltpu.VMEM((pairs,) + square, jnp.bfloat16),
        ],
        compiler_params=pltpu.CompilerParams(vmem_limit_bytes=40 * 2**20),
        cost_estimate=pl.CostEstimate(
            flops=100_000_000_000, bytes_accessed=8 * 2**20, transcendentals=0
        ),
        name="pivots",
    )(piv, shift, pair)


def solve_kernel(dims, at_ref, pan_ref, oth_ref, inv_ref, car_ref, c_ref, g_ref, p_ref):
    prow, pcol, rows = dims
    n = pl.program_id(0)
    children = pan_ref.shape[3]
    extent = inv_ref.shape[-1]
    row = n * prow + at_ref[0]
    col = (n - rows) * pcol + at_ref[1]
    index = jnp.where(n < rows, row, col)

    def body(source):
        solved = []
        for k in range(PANELS):
            left = jnp.concatenate([source(k, 0, c) for c in range(children)], axis=1)
            right = jnp.concatenate([source(k, 1, c) for c in range(children)], axis=1)
            moved = split(nn(inv_ref[k, 0], right) + nn(inv_ref[k, 1], right))
            value = nt(left, moved[0]) + nt(left, moved[1])
            for kk in range(k):
                slot = PAIRS.index((k, kk))
                value = value - nt(solved[kk], car_ref[slot, 0]) - nt(solved[kk], car_ref[slot, 1])
            value = jnp.where(index > k, value, 0.0)
            solved.append(value.astype(jnp.bfloat16))
            g_ref[0, :, k * extent : (k + 1) * extent] = solved[k]

            @pl.when((at_ref[1] == k) & (n < rows))
            def _(value=value, k=k):
                lower = c_ref[k]
                diagonal = lax.broadcasted_iota(
                    jnp.int32, lower.shape, 0
                ) == lax.broadcasted_iota(jnp.int32, lower.shape, 1)
                scale = jnp.sum(jnp.where(diagonal, lower, 0.0), axis=0, keepdims=True)
                p_ref[0] = jnp.where(index == k, lower, value) * scale

    @pl.when(n < rows)
    def _():
        body(lambda k, side, c: pan_ref[k, 0, side, c])

    @pl.when(n >= rows)
    def _():
        body(lambda k, side, c: oth_ref[0, k, side, c])


def solve(prow, pcol, at, pan, oth, inv, car, lower):
    _, rows, _, children, extent, rank = pan.shape
    cols = oth.shape[0]

    def whole(array):
        return pl.BlockSpec(array.shape, lambda n, at: (0,) * array.ndim)

    return pl.pallas_call(
        functools.partial(solve_kernel, (prow, pcol, rows)),
        out_shape=(
            jax.ShapeDtypeStruct((rows + cols, extent, PANELS * extent), jnp.bfloat16),
            jax.ShapeDtypeStruct((rows, extent, extent), jnp.float32),
        ),
        grid_spec=pltpu.PrefetchScalarGridSpec(
            num_scalar_prefetch=1,
            grid=(rows + cols,),
            in_specs=[
                pl.BlockSpec(
                    (PANELS, 1, 2, children, extent, rank),
                    lambda n, at: (0, jnp.minimum(n, rows - 1), 0, 0, 0, 0),
                ),
                pl.BlockSpec(
                    (1, PANELS, 2, children, extent, rank),
                    lambda n, at: (jnp.maximum(n - rows, 0), 0, 0, 0, 0, 0),
                ),
                whole(inv),
                whole(car),
                whole(lower),
            ],
            out_specs=(
                pl.BlockSpec((1, extent, PANELS * extent), lambda n, at: (n, 0, 0)),
                pl.BlockSpec(
                    (1, extent, extent),
                    lambda n, at: (jnp.where(at[1] < PANELS, jnp.minimum(n, rows - 1), 0), 0, 0),
                ),
            ),
        ),
        compiler_params=pltpu.CompilerParams(vmem_limit_bytes=56 * 2**20),
        cost_estimate=pl.CostEstimate(
            flops=22_000_000_000, bytes_accessed=40 * 2**20, transcendentals=0
        ),
        name="solve",
    )(at, pan, oth, inv, car, lower)


def diag_kernel(dims, at_ref, rowbuf, pan_ref, own_ref, sums_ref, mine_ref, shift_ref, d_ref):
    prow, pcol, kept = dims
    slot = pl.program_id(0)
    tiles, children, extent = rowbuf.shape[2], rowbuf.shape[3], rowbuf.shape[4]
    q = at_ref[1]

    @pl.when(at_ref[0] == lax.rem(q, prow))
    def _():
        eye = lax.broadcasted_iota(jnp.int32, (extent, extent), 0) == lax.broadcasted_iota(
            jnp.int32, (extent, extent), 1
        )
        total = mine_ref[0] + jnp.where(eye, shift_ref[0], 0.0)
        for s in range(sums_ref.shape[0]):
            total = total + sums_ref[s, 0]
        for t in range(tiles):
            own = jnp.concatenate([own_ref[0, t, c] for c in range(children)], axis=1)
            if t > 0:
                total = total + nt(own, own)
            else:
                total = total + jnp.where(q >= PANELS, nt(own, own), 0.0)
        for k in range(PANELS):
            tile = jnp.concatenate([pan_ref[k, 0, 0, c] for c in range(children)], axis=1)
            total = total + nt(tile, tile)
        d_ref[0] = total
        for origin in range(pcol):
            for t in range(tiles):
                if t == 0 and origin < PANELS:
                    continue

                @pl.when((q != origin) & (t * pcol < slot * pcol + q))
                def _():
                    tile = jnp.concatenate(
                        [rowbuf[0, origin, t, c] for c in range(children)], axis=1
                    )
                    d_ref[0] += nt(tile, tile)


def diag(prow, pcol, at, rowbuf, pan, rowtiles, sumbuf, sums, shift):
    cols, _, tiles, children, extent, rank = rowbuf.shape
    kept = rowtiles.shape[0]
    others = sumbuf.shape[0]

    def row(slot, at):
        return (slot * pcol + at[1]) // prow

    return pl.pallas_call(
        functools.partial(diag_kernel, (prow, pcol, kept)),
        out_shape=jax.ShapeDtypeStruct((cols, extent, extent), jnp.float32),
        grid_spec=pltpu.PrefetchScalarGridSpec(
            num_scalar_prefetch=1,
            grid=(cols,),
            in_specs=[
                pl.BlockSpec(
                    (1, pcol, tiles, children, extent, rank), lambda s, at: (s, 0, 0, 0, 0, 0)
                ),
                pl.BlockSpec(
                    (PANELS, 1, 1, children, extent, rank),
                    lambda s, at: (0, row(s, at), 0, 0, 0, 0),
                ),
                pl.BlockSpec(
                    (1, tiles, children, extent, rank), lambda s, at: (row(s, at), 0, 0, 0, 0)
                ),
                pl.BlockSpec((others, 1, extent, extent), lambda s, at: (0, s, 0, 0)),
                pl.BlockSpec((1, extent, extent), lambda s, at: (s, 0, 0)),
                pl.BlockSpec((1, 1, extent), lambda s, at: (s * pcol + at[1], 0, 0)),
            ],
            out_specs=pl.BlockSpec((1, extent, extent), lambda s, at: (s, 0, 0)),
        ),
        compiler_params=pltpu.CompilerParams(vmem_limit_bytes=60 * 2**20),
        cost_estimate=pl.CostEstimate(
            flops=6_000_000_000, bytes_accessed=24 * 2**20, transcendentals=0
        ),
        name="diag",
    )(at, rowbuf, pan, rowtiles, sumbuf, sums, shift)


def finish_kernel(dims, at_ref, rank_ref, u_ref, v_ref, g_ref, h_ref, d_ref, p_ref, o_ref):
    prow, pcol = dims
    r = pl.program_id(0)
    children, cols = u_ref.shape[0], u_ref.shape[3]
    extent, rank_max = u_ref.shape[-2:]
    pieces = extent // STEP
    lane = lax.broadcasted_iota(jnp.int32, (1, rank_max), 1)
    i = r * prow + at_ref[0]

    for t in range(cols):
        j = t * pcol + at_ref[1]

        def put(value, t=t):
            for s in range(pieces):
                o_ref[pl.ds(t * pieces + s, extent, stride=cols * pieces), :] = value[
                    :, s * STEP : (s + 1) * STEP
                ]

        @pl.when(i < j)
        def _():
            put(jnp.zeros((extent, extent), jnp.float32))

        if t == 0:

            @pl.when((i >= j) & (j < PANELS))
            def _():
                put(p_ref[0])

        def total(t=t):
            left, right = [], []
            for c in range(children):
                rank = rank_ref[(c * pl.num_programs(0) + r) * cols + t]
                keep = (lane < rank).astype(jnp.bfloat16)
                left.append(u_ref[c, 0, 0, t, 0])
                right.append(v_ref[c, 0, 0, t, 0] * keep)
            value = nt(jnp.concatenate(left, axis=1), jnp.concatenate(right, axis=1))
            return value - nt(g_ref[0], h_ref[t])

        @pl.when((i > j) & (j >= PANELS))
        def _():
            put(total())

        @pl.when((i == j) & (j >= PANELS))
        def _():
            put(total() + d_ref[t])


def finish(prow, pcol, at, ranks, child_u, child_v, wide, diags, panels):
    children, rows, _, cols, _, extent, rank = child_u.shape
    width = wide.shape[-1]
    lines = extent * cols * extent // STEP
    tile = pl.BlockSpec(
        (children, 1, 1, cols, 1, extent, rank), lambda r, at, ranks: (0, r, 0, 0, 0, 0, 0)
    )
    return pl.pallas_call(
        functools.partial(finish_kernel, (prow, pcol)),
        out_shape=jax.ShapeDtypeStruct((rows * lines, STEP), jnp.float32),
        grid_spec=pltpu.PrefetchScalarGridSpec(
            num_scalar_prefetch=2,
            grid=(rows,),
            in_specs=[
                tile,
                tile,
                pl.BlockSpec((1, extent, width), lambda r, at, ranks: (r, 0, 0)),
                pl.BlockSpec((cols, extent, width), lambda r, at, ranks: (rows // cols, 0, 0)),
                pl.BlockSpec((cols, extent, extent), lambda r, at, ranks: (0, 0, 0)),
                pl.BlockSpec(
                    (1, extent, extent),
                    lambda r, at, ranks: (jnp.where(at[1] < PANELS, r, 0), 0, 0),
                ),
            ],
            out_specs=pl.BlockSpec((lines, STEP), lambda r, at, ranks: (r, 0)),
        ),
        compiler_params=pltpu.CompilerParams(vmem_limit_bytes=56 * 2**20),
        cost_estimate=pl.CostEstimate(
            flops=2 * rows * cols * extent * extent * (width + children * rank),
            bytes_accessed=50 * 2**20,
            transcendentals=0,
        ),
        name="finish",
    )(at, ranks, child_u, child_v, wide, wide, diags, panels)


def on_device(prow, pcol, child_u, child_v, child_rank, diag_shift):
    own_row, own_column = lax.axis_index("prow"), lax.axis_index("pcol")
    children, rows, _, cols, _, extent, rank = child_u.shape
    kept = cols * pcol // prow
    tiles = cols
    at = jnp.stack([own_row, own_column]).astype(jnp.int32)
    ranks = child_rank.reshape(-1)
    shift = diag_shift[:, None, :]
    pan, sums, rowtiles = prep(prow, pcol, kept, tiles, at, ranks, child_u, child_v)
    pan, oth, rowbuf, sumbuf, piv, pair = exchange(prow, pcol, pan, sums, rowtiles)
    lower, inv, car = pivots(piv.reshape(PANELS, extent, extent), shift[:PANELS], pair)
    wide, panels = solve(prow, pcol, at, pan, oth, inv, car, lower)
    diags = diag(prow, pcol, at, rowbuf, pan, rowtiles, sumbuf, sums, shift)
    out = finish(prow, pcol, at, ranks, child_u, child_v, wide, diags, panels)
    return out.reshape(rows, 1, extent, cols, 1, extent)


def solution(mesh):
    placed = (
        P(None, None, "prow", None, "pcol", None, None),
        P(None, None, "prow", None, "pcol", None, None),
        P(None, None, "prow", None, "pcol"),
        P(),
    )
    return jax.shard_map(
        functools.partial(on_device, mesh.shape["prow"], mesh.shape["pcol"]),
        mesh=mesh,
        in_specs=placed,
        out_specs=P(None, "prow", None, None, "pcol", None),
        check_vma=False,
    )
```

```python
import functools

import jax
import jax.numpy as jnp
from jax import lax
from jax.experimental import pallas as pl
from jax.experimental.pallas import tpu as pltpu
from jax.sharding import PartitionSpec as P

PANELS = 2
STEP = 128
SUB = 8
PAIRS = [(m, k) for k in range(PANELS) for m in range(k + 1, PANELS)]
MESH = pl.DeviceIdType.MESH
ANY = pl.BlockSpec(memory_space=pl.ANY)


def nt(a, b, precision=None):
    return lax.dot_general(
        a, b, (((1,), (1,)), ((), ())), preferred_element_type=jnp.float32, precision=precision
    )


def nn(a, b, precision=None):
    return lax.dot_general(
        a, b, (((1,), (0,)), ((), ())), preferred_element_type=jnp.float32, precision=precision
    )


def split(value):
    high = value.astype(jnp.bfloat16)
    low = (value - high.astype(jnp.float32)).astype(jnp.bfloat16)
    return high, low


def prep_kernel(dims, at_ref, rank_ref, u_ref, v_ref, pan_ref, sum_ref, row_ref):
    prow, pcol, kept, tiles = dims
    r = pl.program_id(0)
    children, cols = u_ref.shape[0], u_ref.shape[3]
    rank_max = u_ref.shape[-1]
    lane = lax.broadcasted_iota(jnp.int32, (1, rank_max), 1)

    @pl.when(r == 0)
    def _():
        sum_ref[...] = jnp.zeros_like(sum_ref)

    for t in range(cols):
        left, right = [], []
        for c in range(children):
            rank = rank_ref[(c * pl.num_programs(0) + r) * cols + t]
            keep = (lane < rank).astype(jnp.bfloat16)
            left.append(u_ref[c, 0, 0, t, 0] * keep)
            right.append(v_ref[c, 0, 0, t, 0] * keep)
        if t == 0:
            for c in range(children):
                pan_ref[0, 0, 0, c] = left[c]
                pan_ref[0, 0, 1, c] = right[c]
        if t < tiles:

            @pl.when(r < kept)
            def _(left=left, t=t):
                for c in range(children):
                    row_ref[0, t, c] = left[c]

        wide = jnp.concatenate(right, axis=1)
        sum_ref[t] += nt(wide, wide)
        i = r * prow + at_ref[0]
        j = t * pcol + at_ref[1]

        @pl.when((i == j) & (j < PANELS))
        def _(left=left, wide=wide, t=t):
            sum_ref[t] += nt(jnp.concatenate(left, axis=1), wide)


def prep(prow, pcol, kept, tiles, at, ranks, child_u, child_v):
    children, rows, _, cols, _, extent, rank = child_u.shape
    tile = pl.BlockSpec(
        (children, 1, 1, cols, 1, extent, rank), lambda r, at, ranks: (0, r, 0, 0, 0, 0, 0)
    )
    return pl.pallas_call(
        functools.partial(prep_kernel, (prow, pcol, kept, tiles)),
        out_shape=(
            jax.ShapeDtypeStruct((PANELS, rows, 2, children, extent, rank), jnp.bfloat16),
            jax.ShapeDtypeStruct((cols, extent, extent), jnp.float32),
            jax.ShapeDtypeStruct((kept, tiles, children, extent, rank), jnp.bfloat16),
        ),
        grid_spec=pltpu.PrefetchScalarGridSpec(
            num_scalar_prefetch=2,
            grid=(rows,),
            in_specs=[tile, tile],
            out_specs=(
                pl.BlockSpec(
                    (1, 1, 2, children, extent, rank),
                    lambda r, at, ranks: (lax.rem(at[1], PANELS), r, 0, 0, 0, 0),
                ),
                pl.BlockSpec((cols, extent, extent), lambda r, at, ranks: (0, 0, 0)),
                pl.BlockSpec(
                    (1, tiles, children, extent, rank),
                    lambda r, at, ranks: (jnp.minimum(r, kept - 1), 0, 0, 0, 0),
                ),
            ),
        ),
        compiler_params=pltpu.CompilerParams(vmem_limit_bytes=40 * 2**20),
        cost_estimate=pl.CostEstimate(
            flops=2 * rows * cols * extent * extent * children * rank,
            bytes_accessed=18 * 2**20,
            transcendentals=0,
        ),
        name="prep",
    )(at, ranks, child_u, child_v)


def factor_tile(tile):
    row = lax.broadcasted_iota(jnp.int32, (STEP, STEP), 0)
    lane = lax.broadcasted_iota(jnp.int32, (STEP, STEP), 1)
    left, right = tile, (row == lane).astype(jnp.float32)
    uppers, inverses = [], []
    for base in range(0, STEP, SUB):
        extent = STEP - base
        index = lax.broadcasted_iota(jnp.int32, (extent, STEP), 0)
        weights = [
            jnp.broadcast_to(left[:, base + j : base + j + 1], (extent, STEP)) for j in range(SUB)
        ]
        for j in range(SUB):
            inverse = 1.0 / weights[j][j : j + 1]
            weight = jnp.where(index > j, weights[j], 0.0)
            row_left = left[j : j + 1] * inverse
            row_right = right[j : j + 1] * inverse
            for k in range(j + 1, SUB):
                weights[k] = weights[k] - weight * (weights[k][j : j + 1] * inverse)
            left = left - weight * row_left
            right = right - weight * row_right
        uppers.append(left[:SUB])
        inverses.append(right[:SUB])
        left, right = left[SUB:], right[SUB:]
    return jnp.concatenate(uppers, axis=0), jnp.concatenate(inverses, axis=0)


def factor_block(block, w_ref, e_ref, c_ref, y_ref, between):
    extent = w_ref.shape[0]
    exact = lax.Precision.HIGHEST
    base = pl.multiple_of(block * STEP, STEP)
    here = pl.ds(base, STEP)
    upper, lower_inverse = factor_tile(w_ref[here, here])
    between()
    tile_row = lax.broadcasted_iota(jnp.int32, (STEP, STEP), 0)
    tile_col = lax.broadcasted_iota(jnp.int32, (STEP, STEP), 1)
    pivots = jnp.sum(jnp.where(tile_row == tile_col, upper, 0.0), axis=1, keepdims=True)
    root = jnp.sqrt(pivots)
    pivot_factor = (jnp.where(tile_row <= tile_col, upper, 0.0) / root).T
    pivot_inverse = lower_inverse / root
    panel = nt(w_ref[:, here], pivot_inverse, exact)
    below = lax.broadcasted_iota(jnp.int32, (extent, STEP), 0) >= base + STEP
    panel = jnp.where(below, panel, 0.0)
    c_ref[:, here] = panel
    c_ref[here, here] = pivot_factor
    solved = nn(pivot_inverse, e_ref[here, :], exact)
    y_ref[here, :] = solved
    w_ref[...] -= nt(panel, panel, exact)
    e_ref[...] -= nn(panel, solved, exact)


def exchange_kernel(
    dims, pan_in, sum_ref, row_ref, shift_ref, pan, oth, rowbuf, sumbuf, piv, pair, wide_ref,
    panel_ref, *scratch
):
    prow, pcol, rows, cols, kept, tiles, children = dims
    (part, total, pivots, pairs, w_ref, e_ref, y_ref, c_ref, inv_ref, car_ref, g_ref,
     scale_ref, tile_ref, solved_ref, scaled_ref,
     local, part_s, part_r, sum_s, sum_r, row_s, row_r, chain_s, chain_r, cross_s, cross_r,
     oth_s, oth_r, pair_s, pair_r, gat_s, gat_r, piv_l, pair_l, load_l, store_l, scaled_l) = scratch
    del pan_in
    p, q = lax.axis_index("prow"), lax.axis_index("pcol")
    z, y = q // PANELS, lax.rem(q, PANELS)
    depth = pcol // PANELS
    home = lax.rem(q, prow)
    extent = sum_ref.shape[-1]
    band = extent // prow
    blocks = extent // STEP
    last = 2 * rows
    near = 2 * kept
    early = 4
    turns = PANELS * blocks

    barrier = pltpu.get_barrier_semaphore()
    for d in range(1, pcol):
        pl.semaphore_signal(
            barrier, inc=1, device_id={"pcol": lax.rem(q + d, pcol)}, device_id_type=MESH
        )
    for d in range(1, prow):
        pl.semaphore_signal(
            barrier, inc=1, device_id={"prow": lax.rem(p + d, prow)}, device_id_type=MESH
        )
    pl.semaphore_wait(barrier, pcol + prow - 2)

    def send(src, dst, send_sem, recv_sem, **target):
        return pltpu.make_async_remote_copy(
            src_ref=src, dst_ref=dst, send_sem=send_sem, recv_sem=recv_sem,
            device_id=target, device_id_type=MESH,
        )

    def bands(o):
        return pl.ds(pl.multiple_of(o * band, 8), band)

    def part_copy(d):
        s = lax.rem(p + d, prow)
        return send(
            sum_ref.at[0, bands(s)], part.at[d], part_s.at[d - 1], part_r.at[d - 1], prow=s
        )

    def part_own():
        return pltpu.make_async_copy(sum_ref.at[0, bands(p)], part.at[0], local.at[0])

    def sum_copy():
        d = lax.rem(home + prow - p, prow) - 1
        return send(sum_ref, sumbuf.at[d], sum_s, sum_r.at[d], prow=home)

    def sum_arrival(d):
        return send(sum_ref, sumbuf.at[d], sum_s, sum_r.at[d], prow=home)

    def reach(r):
        return sum(1 for t in range(tiles) if t * pcol < (r + 1) * prow)

    def row_copy(r, first):
        i = r * prow + p
        owner, slot = lax.rem(i, pcol), i // pcol
        window = pl.ds(first, reach(r) - first)
        return send(
            row_ref.at[r, window], rowbuf.at[slot, q, window], row_s.at[r], row_r.at[slot, q],
            pcol=owner,
        )

    def row_arrival(slot, origin, r, first):
        window = pl.ds(first, reach(r) - first)
        return send(
            row_ref.at[r, window], rowbuf.at[slot, origin, window], row_s.at[r],
            row_r.at[slot, origin], pcol=origin,
        )

    def chunk(which, n):
        if isinstance(n, int) and n == last:
            return piv.at[which, bands(p)]
        return pan.at[which, lax.div(n, 2), lax.rem(n, 2)]

    def chain_copy(n):
        ref = chunk(y, n)
        return send(ref, ref, chain_s.at[n], chain_r.at[n], pcol=q + PANELS)

    def cross_copy(n, which):
        ref = chunk(which, n)
        return send(ref, ref, cross_s.at[n], cross_r.at[n], pcol=q + 1 - 2 * y)

    def needed(n, plane):
        if isinstance(n, int) and n == last:
            return plane >= 0
        i = lax.div(n, 2) * prow + p
        used = i >= plane * PANELS
        for m, _ in PAIRS:
            used = used | (i == m)
        return used

    def step(n):
        @pl.when((z > 0) & needed(n, z))
        def _():
            chain_copy(n).wait_recv()

        @pl.when((z < depth - 1) & needed(n, z + 1))
        def _():
            chain_copy(n).start()

        @pl.when(needed(n, z))
        def _():
            cross_copy(n, y).start()

    def cross_arrival(n):
        @pl.when(needed(n, z))
        def _():
            cross_copy(n, 1 - y).wait_recv()

    def oth_row(t):
        return (t * pcol + q) // prow

    def oth_copy(t, k, d):
        n = t * PANELS + k
        return send(
            pan.at[k, oth_row(t)], oth.at[t, k], oth_s.at[n, d - 1], oth_r.at[n],
            prow=lax.rem(p + d, prow),
        )

    def pair_copy(n, d):
        m, k = PAIRS[n]
        return send(
            pan.at[k, m // prow], pair.at[n], pair_s.at[n, d - 1], pair_r.at[n],
            prow=lax.rem(p + d, prow),
        )

    def gat_copy(k, d):
        ref = piv.at[k, bands(p)]
        return send(
            ref, ref, gat_s.at[k, d - 1], gat_r.at[k, d - 1], prow=lax.rem(p + d, prow)
        )

    def gat_arrival(k, d):
        o = lax.rem(p + prow - d, prow)
        ref = piv.at[k, bands(o)]
        return send(ref, ref, gat_s.at[k, d - 1], gat_r.at[k, d - 1], prow=o)

    @pl.when(z == 0)
    def _():
        for d in range(1, prow):
            part_copy(d).start()
        part_own().start()

    step(0)
    step(1)

    @pl.when(z == 0)
    def _():
        part_own().wait()
        for d in range(1, prow):
            part_copy(d).wait_recv()
        value = part[0]
        for d in range(1, prow):
            value = value + part[d]
        total[...] = value
        out = pltpu.make_async_copy(total, piv.at[y, bands(p)], local.at[1])
        out.start()
        out.wait()

    step(last)
    cross_arrival(last)
    for k in range(PANELS):
        for d in range(1, prow):
            gat_copy(k, d).start()

    step(2)
    for n in range(2):
        cross_arrival(n)
    for n, (m, k) in enumerate(PAIRS):

        @pl.when(p == m % prow)
        def _():
            for d in range(1, prow):
                pair_copy(n, d).start()

    @pl.when(p != home)
    def _():
        sum_copy().start()

    for r in range(kept):
        owner = lax.rem(r * prow + p, pcol)

        @pl.when((q != owner) & (z > 0))
        def _():
            row_copy(r, 0).start()

        if reach(r) > 1:

            @pl.when((q != owner) & (z == 0))
            def _():
                row_copy(r, 1).start()

    step(3)
    for k in range(PANELS):
        for d in range(1, prow):
            gat_arrival(k, d).wait_recv()
    loads = [pltpu.make_async_copy(piv.at[k], pivots.at[k], piv_l.at[k]) for k in range(PANELS)]
    for load in loads:
        load.start()
    for load in loads:
        load.wait()

    def near_wait():
        for n in range(2, near):
            cross_arrival(n)

        @pl.when(p == home)
        def _():
            for t in range(cols):
                for k in range(PANELS):
                    for d in range(1, prow):
                        oth_copy(t, k, d).start()

    eye = lax.broadcasted_iota(jnp.int32, (extent, extent), 0) == lax.broadcasted_iota(
        jnp.int32, (extent, extent), 1
    )

    def joined(n, side):
        return jnp.concatenate([pairs[n, side, c] for c in range(children)], axis=1)

    @pl.loop(0, turns)
    def _(turn):
        k, block = lax.div(turn, blocks), lax.rem(turn, blocks)

        @pl.when(block == 0)
        def _():
            w_ref[...] = pivots[k] + jnp.where(eye, shift_ref[pl.ds(k, 1), :], 0.0)
            for n, (m, _) in enumerate(PAIRS):

                @pl.when(k == m)
                def _():
                    left = joined(n, 0)
                    g = g_ref[n]
                    w_ref[...] += nt(left, left) - nt(g, g)

            e_ref[...] = eye.astype(jnp.float32)

        def service():
            @pl.when(turn + early < last)
            def _():
                step(turn + early)

        factor_block(block, w_ref, e_ref, c_ref.at[k], y_ref, service)

        @pl.when(turn == turns - 2)
        def _():
            near_wait()

        @pl.when(turn == blocks - 1)
        def _():
            for n, (m, kk) in enumerate(PAIRS):

                @pl.when(p == m % prow)
                def _():
                    load = pltpu.make_async_copy(pan.at[kk, m // prow], pairs.at[n], pair_l.at[n])
                    load.start()
                    load.wait()

                @pl.when(p != m % prow)
                def _():
                    pair_copy(n, 1).wait_recv()
                    load = pltpu.make_async_copy(pair.at[n], pairs.at[n], pair_l.at[n])
                    load.start()
                    load.wait()

        @pl.when(block == blocks - 1)
        def _():
            high, low = split(y_ref[...])
            inv_ref[k, 0] = high
            inv_ref[k, 1] = low
            scale_ref[k] = jnp.sum(jnp.where(eye, c_ref[k], 0.0), axis=0, keepdims=True)

            for n, (m, kk) in enumerate(PAIRS):

                @pl.when(k == kk)
                def _():
                    right = joined(n, 1)
                    moved = split(nn(high, right) + nn(low, right))
                    left = joined(n, 0)
                    value = nt(left, moved[0]) + nt(left, moved[1])
                    for o, (mo, ko) in enumerate(PAIRS):
                        if mo == m and ko < kk:
                            slot = PAIRS.index((kk, ko))
                            for s in range(2):
                                value = value - nt(g_ref[o], car_ref[slot, s])
                    g_ref[n] = value.astype(jnp.bfloat16)

                @pl.when(k == m)
                def _():
                    g = g_ref[n]
                    one, two = split(nn(high, g) + nn(low, g))
                    car_ref[n, 0] = one
                    car_ref[n, 1] = two

    turn_at = max(rows - 2, kept)
    count = rows + cols
    left_over = max(last - early - turns, 0)
    pace = -(-left_over // rows)

    def is_row(s):
        return (s < turn_at) | (s >= turn_at + cols)

    def row_of(s):
        return jnp.where(s < turn_at, s, s - cols)

    def row_load(s):
        r = row_of(s)
        return pltpu.make_async_copy(
            pan.at[:, r], tile_ref.at[lax.rem(s, 2)], load_l.at[lax.rem(s, 2)]
        )

    def near_load(s):
        t = s - turn_at
        return pltpu.make_async_copy(
            oth.at[t], tile_ref.at[lax.rem(s, 2)], load_l.at[lax.rem(s, 2)]
        )

    def own_load(s, k):
        t = s - turn_at
        return pltpu.make_async_copy(
            pan.at[k, oth_row(t)], tile_ref.at[lax.rem(s, 2), k],
            local.at[2 + t * PANELS + k],
        )

    def begin(s):
        @pl.when(is_row(s))
        def _():
            r = row_of(s)

            @pl.when(r >= kept)
            def _():
                cross_arrival(2 * r)
                cross_arrival(2 * r + 1)

            row_load(s).start()

        @pl.when(jnp.logical_not(is_row(s)))
        def _():
            @pl.when(p == home)
            def _():
                for k in range(PANELS):
                    own_load(s, k).start()

            @pl.when(p != home)
            def _():
                for k in range(PANELS):
                    n = (s - turn_at) * PANELS + k
                    send(
                        oth.at[s - turn_at, k], oth.at[s - turn_at, k], oth_s.at[n, 0],
                        oth_r.at[n], prow=home,
                    ).wait_recv()
                near_load(s).start()

    def ready(s):
        @pl.when(is_row(s))
        def _():
            row_load(s).wait()

        @pl.when(jnp.logical_not(is_row(s)) & (p == home))
        def _():
            for k in range(PANELS):
                own_load(s, k).wait()

        @pl.when(jnp.logical_not(is_row(s)) & (p != home))
        def _():
            near_load(s).wait()

    def store(s):
        place = jnp.where(is_row(s), row_of(s), rows + s - turn_at)
        return pltpu.make_async_copy(
            solved_ref.at[lax.rem(s, 2)], wide_ref.at[place], store_l.at[lax.rem(s, 2)]
        )

    def scaled_store(s):
        return pltpu.make_async_copy(
            scaled_ref.at[lax.rem(s, 2)], panel_ref.at[row_of(s)], scaled_l.at[lax.rem(s, 2)]
        )

    begin(0)

    @pl.loop(0, count)
    def _(s):
        for c in range(pace):
            n = early + turns + pace * s + c

            @pl.when(n < last)
            def _(n=n):
                step(n)

        @pl.when(s + 1 < count)
        def _():
            begin(s + 1)

        ready(s)

        @pl.when(s >= 2)
        def _():
            store(s - 2).wait()

            @pl.when(is_row(s - 2) & (q < PANELS))
            def _():
                scaled_store(s - 2).wait()

        slot = lax.rem(s, 2)
        index = jnp.where(is_row(s), row_of(s) * prow + p, (s - turn_at) * pcol + q)
        solved = []
        for k in range(PANELS):
            left = jnp.concatenate([tile_ref[slot, k, 0, c] for c in range(children)], axis=1)
            right = jnp.concatenate([tile_ref[slot, k, 1, c] for c in range(children)], axis=1)
            moved = split(nn(inv_ref[k, 0], right) + nn(inv_ref[k, 1], right))
            value = nt(left, moved[0]) + nt(left, moved[1])
            for kk in range(k):
                pos = PAIRS.index((k, kk))
                value = value - nt(solved[kk], car_ref[pos, 0]) - nt(solved[kk], car_ref[pos, 1])
            value = jnp.where(index > k, value, 0.0)
            solved.append(value.astype(jnp.bfloat16))
            solved_ref[slot, :, k * extent : (k + 1) * extent] = solved[k]

            @pl.when((q == k) & is_row(s))
            def _(value=value, k=k):
                scaled_ref[slot] = jnp.where(index == k, c_ref[k], value) * scale_ref[k]

        store(s).start()

        @pl.when(is_row(s) & (q < PANELS))
        def _():
            scaled_store(s).start()

    for s in range(count - 2, count):
        store(s).wait()

        @pl.when(is_row(s) & (q < PANELS))
        def _():
            scaled_store(s).wait()

    for k in range(PANELS):
        for d in range(1, prow):
            gat_copy(k, d).wait_send()
    for n, (m, k) in enumerate(PAIRS):

        @pl.when(p == m % prow)
        def _():
            for d in range(1, prow):
                pair_copy(n, d).wait_send()

    @pl.when(p == home)
    def _():
        for t in range(cols):
            for k in range(PANELS):
                for d in range(1, prow):
                    oth_copy(t, k, d).wait_send()
        for d in range(prow - 1):
            sum_arrival(d).wait_recv()
        for slot in range(cols):
            for origin in range(pcol):

                @pl.when(q != origin)
                def _():
                    low = slot * pcol // prow
                    first = 1 if origin < PANELS else 0
                    if reach(low) > first:
                        row_arrival(slot, origin, low, first).wait_recv()

    @pl.when(p != home)
    def _():
        sum_copy().wait_send()

    @pl.when(z == 0)
    def _():
        for d in range(1, prow):
            part_copy(d).wait_send()

    for r in range(kept):
        owner = lax.rem(r * prow + p, pcol)

        @pl.when((q != owner) & (z > 0))
        def _():
            row_copy(r, 0).wait_send()

        if reach(r) > 1:

            @pl.when((q != owner) & (z == 0))
            def _():
                row_copy(r, 1).wait_send()

    for n in range(last + 1):

        @pl.when((z < depth - 1) & needed(n, z + 1))
        def _():
            chain_copy(n).wait_send()

        @pl.when(needed(n, z))
        def _():
            cross_copy(n, y).wait_send()


def exchange(prow, pcol, pan, sums, rowtiles, shift):
    _, rows, _, children, extent, rank = pan.shape
    cols = sums.shape[0]
    kept, tiles = rowtiles.shape[:2]
    band = extent // prow
    pairs = max(len(PAIRS), 1)
    dma = pltpu.SemaphoreType.DMA
    square = (extent, extent)
    narrow = pan.dtype
    return pl.pallas_call(
        functools.partial(exchange_kernel, (prow, pcol, rows, cols, kept, tiles, children)),
        out_shape=(
            jax.ShapeDtypeStruct(pan.shape, narrow),
            jax.ShapeDtypeStruct((cols, PANELS, 2, children, extent, rank), narrow),
            jax.ShapeDtypeStruct((cols, pcol, tiles, children, extent, rank), narrow),
            jax.ShapeDtypeStruct((prow - 1, cols) + square, jnp.float32),
            jax.ShapeDtypeStruct((PANELS,) + square, jnp.float32),
            jax.ShapeDtypeStruct((pairs, 2, children, extent, rank), narrow),
            jax.ShapeDtypeStruct((rows + cols, extent, PANELS * extent), narrow),
            jax.ShapeDtypeStruct((rows,) + square, jnp.float32),
        ),
        in_specs=[ANY, ANY, ANY, pl.BlockSpec(memory_space=pltpu.VMEM)],
        out_specs=(ANY,) * 8,
        scratch_shapes=[
            pltpu.VMEM((prow, band, extent), jnp.float32),
            pltpu.VMEM((band, extent), jnp.float32),
            pltpu.VMEM((PANELS,) + square, jnp.float32),
            pltpu.VMEM((pairs, 2, children, extent, rank), narrow),
            pltpu.VMEM(square, jnp.float32),
            pltpu.VMEM(square, jnp.float32),
            pltpu.VMEM(square, jnp.float32),
            pltpu.VMEM((PANELS,) + square, jnp.float32),
            pltpu.VMEM((PANELS, 2) + square, narrow),
            pltpu.VMEM((pairs, 2) + square, narrow),
            pltpu.VMEM((pairs,) + square, narrow),
            pltpu.VMEM((PANELS, 1, extent), jnp.float32),
            pltpu.VMEM((2, PANELS, 2, children, extent, rank), narrow),
            pltpu.VMEM((2, extent, PANELS * extent), narrow),
            pltpu.VMEM((2,) + square, jnp.float32),
            dma((2 + cols * PANELS,)),
            dma((prow - 1,)),
            dma((prow - 1,)),
            dma,
            dma((prow - 1,)),
            dma((kept,)),
            dma((cols, pcol)),
            dma((2 * rows + 1,)),
            dma((2 * rows + 1,)),
            dma((2 * rows + 1,)),
            dma((2 * rows + 1,)),
            dma((cols * PANELS, prow - 1)),
            dma((cols * PANELS,)),
            dma((pairs, prow - 1)),
            dma((pairs,)),
            dma((PANELS, prow - 1)),
            dma((PANELS, prow - 1)),
            dma((PANELS,)),
            dma((pairs,)),
            dma((2,)),
            dma((2,)),
            dma((2,)),
        ],
        input_output_aliases={0: 0},
        compiler_params=pltpu.CompilerParams(
            collective_id=0, has_side_effects=True, vmem_limit_bytes=67_043_328
        ),
        cost_estimate=pl.CostEstimate(
            flops=120_000_000_000, bytes_accessed=90 * 2**20, transcendentals=0
        ),
        name="exchange",
    )(pan, sums, rowtiles, shift)


def diag_kernel(dims, at_ref, rowbuf, pan_ref, own_ref, sums_ref, mine_ref, shift_ref, d_ref):
    prow, pcol, kept = dims
    slot = pl.program_id(0)
    tiles, children, extent = rowbuf.shape[2], rowbuf.shape[3], rowbuf.shape[4]
    q = at_ref[1]

    @pl.when(at_ref[0] == lax.rem(q, prow))
    def _():
        eye = lax.broadcasted_iota(jnp.int32, (extent, extent), 0) == lax.broadcasted_iota(
            jnp.int32, (extent, extent), 1
        )
        shift = shift_ref[pl.ds(slot * pcol + q, 1), :]
        total = mine_ref[0] + jnp.where(eye, shift, 0.0)
        for s in range(sums_ref.shape[0]):
            total = total + sums_ref[s, 0]
        for t in range(tiles):
            own = jnp.concatenate([own_ref[0, t, c] for c in range(children)], axis=1)
            if t > 0:
                total = total + nt(own, own)
            else:
                total = total + jnp.where(q >= PANELS, nt(own, own), 0.0)
        for k in range(PANELS):
            tile = jnp.concatenate([pan_ref[k, 0, 0, c] for c in range(children)], axis=1)
            total = total + nt(tile, tile)
        d_ref[0] = total
        for origin in range(pcol):
            for t in range(tiles):
                if t == 0 and origin < PANELS:
                    continue

                @pl.when((q != origin) & (t * pcol < slot * pcol + q))
                def _():
                    tile = jnp.concatenate(
                        [rowbuf[0, origin, t, c] for c in range(children)], axis=1
                    )
                    d_ref[0] += nt(tile, tile)


def diag(prow, pcol, at, rowbuf, pan, rowtiles, sumbuf, sums, shift):
    cols, _, tiles, children, extent, rank = rowbuf.shape
    kept = rowtiles.shape[0]
    others = sumbuf.shape[0]

    def row(slot, at):
        return (slot * pcol + at[1]) // prow

    return pl.pallas_call(
        functools.partial(diag_kernel, (prow, pcol, kept)),
        out_shape=jax.ShapeDtypeStruct((cols, extent, extent), jnp.float32),
        grid_spec=pltpu.PrefetchScalarGridSpec(
            num_scalar_prefetch=1,
            grid=(cols,),
            in_specs=[
                pl.BlockSpec(
                    (1, pcol, tiles, children, extent, rank), lambda s, at: (s, 0, 0, 0, 0, 0)
                ),
                pl.BlockSpec(
                    (PANELS, 1, 1, children, extent, rank),
                    lambda s, at: (0, row(s, at), 0, 0, 0, 0),
                ),
                pl.BlockSpec(
                    (1, tiles, children, extent, rank), lambda s, at: (row(s, at), 0, 0, 0, 0)
                ),
                pl.BlockSpec((others, 1, extent, extent), lambda s, at: (0, s, 0, 0)),
                pl.BlockSpec((1, extent, extent), lambda s, at: (s, 0, 0)),
                pl.BlockSpec(shift.shape, lambda s, at: (0, 0)),
            ],
            out_specs=pl.BlockSpec((1, extent, extent), lambda s, at: (s, 0, 0)),
        ),
        compiler_params=pltpu.CompilerParams(vmem_limit_bytes=60 * 2**20),
        cost_estimate=pl.CostEstimate(
            flops=6_000_000_000, bytes_accessed=24 * 2**20, transcendentals=0
        ),
        name="diag",
    )(at, rowbuf, pan, rowtiles, sumbuf, sums, shift)


def finish_kernel(dims, at_ref, rank_ref, u_ref, v_ref, g_ref, h_ref, d_ref, p_ref, o_ref):
    prow, pcol = dims
    r = pl.program_id(0)
    children, cols = u_ref.shape[0], u_ref.shape[3]
    extent, rank_max = u_ref.shape[-2:]
    pieces = extent // STEP
    lane = lax.broadcasted_iota(jnp.int32, (1, rank_max), 1)
    i = r * prow + at_ref[0]

    for t in range(cols):
        j = t * pcol + at_ref[1]

        def put(value, t=t):
            for s in range(pieces):
                o_ref[pl.ds(t * pieces + s, extent, stride=cols * pieces), :] = value[
                    :, s * STEP : (s + 1) * STEP
                ]

        @pl.when(i < j)
        def _():
            put(jnp.zeros((extent, extent), jnp.float32))

        if t == 0:

            @pl.when((i >= j) & (j < PANELS))
            def _():
                put(p_ref[0])

        def total(t=t):
            left, right = [], []
            for c in range(children):
                rank = rank_ref[(c * pl.num_programs(0) + r) * cols + t]
                keep = (lane < rank).astype(jnp.bfloat16)
                left.append(u_ref[c, 0, 0, t, 0])
                right.append(v_ref[c, 0, 0, t, 0] * keep)
            value = nt(jnp.concatenate(left, axis=1), jnp.concatenate(right, axis=1))
            return value - nt(g_ref[0], h_ref[t])

        @pl.when((i > j) & (j >= PANELS))
        def _():
            put(total())

        @pl.when((i == j) & (j >= PANELS))
        def _():
            put(total() + d_ref[t])


def finish(prow, pcol, at, ranks, child_u, child_v, wide, diags, panels):
    children, rows, _, cols, _, extent, rank = child_u.shape
    width = wide.shape[-1]
    lines = extent * cols * extent // STEP
    tile = pl.BlockSpec(
        (children, 1, 1, cols, 1, extent, rank), lambda r, at, ranks: (0, r, 0, 0, 0, 0, 0)
    )
    return pl.pallas_call(
        functools.partial(finish_kernel, (prow, pcol)),
        out_shape=jax.ShapeDtypeStruct((rows * lines, STEP), jnp.float32),
        grid_spec=pltpu.PrefetchScalarGridSpec(
            num_scalar_prefetch=2,
            grid=(rows,),
            in_specs=[
                tile,
                tile,
                pl.BlockSpec((1, extent, width), lambda r, at, ranks: (r, 0, 0)),
                pl.BlockSpec((cols, extent, width), lambda r, at, ranks: (rows // cols, 0, 0)),
                pl.BlockSpec((cols, extent, extent), lambda r, at, ranks: (0, 0, 0)),
                pl.BlockSpec(
                    (1, extent, extent),
                    lambda r, at, ranks: (jnp.where(at[1] < PANELS, r, 0), 0, 0),
                ),
            ],
            out_specs=pl.BlockSpec((lines, STEP), lambda r, at, ranks: (r, 0)),
        ),
        compiler_params=pltpu.CompilerParams(vmem_limit_bytes=56 * 2**20),
        cost_estimate=pl.CostEstimate(
            flops=2 * rows * cols * extent * extent * (width + children * rank),
            bytes_accessed=50 * 2**20,
            transcendentals=0,
        ),
        name="finish",
    )(at, ranks, child_u, child_v, wide, wide, diags, panels)


def on_device(prow, pcol, child_u, child_v, child_rank, diag_shift):
    own_row, own_column = lax.axis_index("prow"), lax.axis_index("pcol")
    children, rows, _, cols, _, extent, rank = child_u.shape
    kept = cols * pcol // prow
    tiles = cols
    at = jnp.stack([own_row, own_column]).astype(jnp.int32)
    ranks = child_rank.reshape(-1)
    pan, sums, rowtiles = prep(prow, pcol, kept, tiles, at, ranks, child_u, child_v)
    pan, _, rowbuf, sumbuf, _, _, wide, panels = exchange(
        prow, pcol, pan, sums, rowtiles, diag_shift
    )
    diags = diag(prow, pcol, at, rowbuf, pan, rowtiles, sumbuf, sums, diag_shift)
    out = finish(prow, pcol, at, ranks, child_u, child_v, wide, diags, panels)
    return out.reshape(rows, 1, extent, cols, 1, extent)


def solution(mesh):
    placed = (
        P(None, None, "prow", None, "pcol", None, None),
        P(None, None, "prow", None, "pcol", None, None),
        P(None, None, "prow", None, "pcol"),
        P(),
    )
    return jax.shard_map(
        functools.partial(on_device, mesh.shape["prow"], mesh.shape["pcol"]),
        mesh=mesh,
        in_specs=placed,
        out_specs=P(None, "prow", None, None, "pcol", None),
        check_vma=False,
    )
```

```python
import functools

import jax
import jax.numpy as jnp
from jax import lax
from jax.experimental import pallas as pl
from jax.experimental.pallas import tpu as pltpu
from jax.sharding import PartitionSpec as P

PANELS = 2
STEP = 128
SUB = 8
PAIRS = [(m, k) for k in range(PANELS) for m in range(k + 1, PANELS)]
MESH = pl.DeviceIdType.MESH
ANY = pl.BlockSpec(memory_space=pl.ANY)


def nt(a, b, precision=None):
    return lax.dot_general(
        a, b, (((1,), (1,)), ((), ())), preferred_element_type=jnp.float32, precision=precision
    )


def nn(a, b, precision=None):
    return lax.dot_general(
        a, b, (((1,), (0,)), ((), ())), preferred_element_type=jnp.float32, precision=precision
    )


def split(value):
    high = value.astype(jnp.bfloat16)
    low = (value - high.astype(jnp.float32)).astype(jnp.bfloat16)
    return high, low


def prep_kernel(dims, at_ref, rank_ref, u_ref, v_ref, pan_ref, sum_ref, row_ref):
    prow, pcol, kept, tiles = dims
    r = pl.program_id(0)
    children, cols = u_ref.shape[0], u_ref.shape[3]
    rank_max = u_ref.shape[-1]
    lane = lax.broadcasted_iota(jnp.int32, (1, rank_max), 1)

    @pl.when(r == 0)
    def _():
        sum_ref[...] = jnp.zeros_like(sum_ref)

    for t in range(cols):
        left, right = [], []
        for c in range(children):
            rank = rank_ref[(c * pl.num_programs(0) + r) * cols + t]
            keep = (lane < rank).astype(jnp.bfloat16)
            left.append(u_ref[c, 0, 0, t, 0] * keep)
            right.append(v_ref[c, 0, 0, t, 0] * keep)
        if t == 0:
            for c in range(children):
                pan_ref[0, 0, 0, c] = left[c]
                pan_ref[0, 0, 1, c] = right[c]
        if t < tiles:

            @pl.when(r < kept)
            def _(left=left, t=t):
                for c in range(children):
                    row_ref[0, t, c] = left[c]

        wide = jnp.concatenate(right, axis=1)
        sum_ref[t] += nt(wide, wide)
        i = r * prow + at_ref[0]
        j = t * pcol + at_ref[1]

        @pl.when((i == j) & (j < PANELS))
        def _(left=left, wide=wide, t=t):
            sum_ref[t] += nt(jnp.concatenate(left, axis=1), wide)


def prep(prow, pcol, kept, tiles, at, ranks, child_u, child_v):
    children, rows, _, cols, _, extent, rank = child_u.shape
    tile = pl.BlockSpec(
        (children, 1, 1, cols, 1, extent, rank), lambda r, at, ranks: (0, r, 0, 0, 0, 0, 0)
    )
    return pl.pallas_call(
        functools.partial(prep_kernel, (prow, pcol, kept, tiles)),
        out_shape=(
            jax.ShapeDtypeStruct((PANELS, rows, 2, children, extent, rank), jnp.bfloat16),
            jax.ShapeDtypeStruct((cols, extent, extent), jnp.float32),
            jax.ShapeDtypeStruct((kept, tiles, children, extent, rank), jnp.bfloat16),
        ),
        grid_spec=pltpu.PrefetchScalarGridSpec(
            num_scalar_prefetch=2,
            grid=(rows,),
            in_specs=[tile, tile],
            out_specs=(
                pl.BlockSpec(
                    (1, 1, 2, children, extent, rank),
                    lambda r, at, ranks: (lax.rem(at[1], PANELS), r, 0, 0, 0, 0),
                ),
                pl.BlockSpec((cols, extent, extent), lambda r, at, ranks: (0, 0, 0)),
                pl.BlockSpec(
                    (1, tiles, children, extent, rank),
                    lambda r, at, ranks: (jnp.minimum(r, kept - 1), 0, 0, 0, 0),
                ),
            ),
        ),
        compiler_params=pltpu.CompilerParams(vmem_limit_bytes=67_043_328),
        cost_estimate=pl.CostEstimate(
            flops=2 * rows * cols * extent * extent * children * rank,
            bytes_accessed=18 * 2**20,
            transcendentals=0,
        ),
        name="prep",
    )(at, ranks, child_u, child_v)


def factor_tile(tile):
    row = lax.broadcasted_iota(jnp.int32, (STEP, STEP), 0)
    lane = lax.broadcasted_iota(jnp.int32, (STEP, STEP), 1)
    left, right = tile, (row == lane).astype(jnp.float32)
    uppers, inverses = [], []
    for base in range(0, STEP, SUB):
        extent = STEP - base
        index = lax.broadcasted_iota(jnp.int32, (extent, STEP), 0)
        weights = [
            jnp.broadcast_to(left[:, base + j : base + j + 1], (extent, STEP)) for j in range(SUB)
        ]
        for j in range(SUB):
            inverse = 1.0 / weights[j][j : j + 1]
            weight = jnp.where(index > j, weights[j], 0.0)
            row_left = left[j : j + 1] * inverse
            row_right = right[j : j + 1] * inverse
            for k in range(j + 1, SUB):
                weights[k] = weights[k] - weight * (weights[k][j : j + 1] * inverse)
            left = left - weight * row_left
            right = right - weight * row_right
        uppers.append(left[:SUB])
        inverses.append(right[:SUB])
        left, right = left[SUB:], right[SUB:]
    return jnp.concatenate(uppers, axis=0), jnp.concatenate(inverses, axis=0)


def factor_block(block, w_ref, e_ref, c_ref, y_ref, between):
    extent = w_ref.shape[0]
    exact = lax.Precision.HIGHEST
    base = pl.multiple_of(block * STEP, STEP)
    here = pl.ds(base, STEP)
    upper, lower_inverse = factor_tile(w_ref[here, here])
    between()
    tile_row = lax.broadcasted_iota(jnp.int32, (STEP, STEP), 0)
    tile_col = lax.broadcasted_iota(jnp.int32, (STEP, STEP), 1)
    pivots = jnp.sum(jnp.where(tile_row == tile_col, upper, 0.0), axis=1, keepdims=True)
    root = jnp.sqrt(pivots)
    pivot_factor = (jnp.where(tile_row <= tile_col, upper, 0.0) / root).T
    pivot_inverse = lower_inverse / root
    panel = nt(w_ref[:, here], pivot_inverse, exact)
    below = lax.broadcasted_iota(jnp.int32, (extent, STEP), 0) >= base + STEP
    panel = jnp.where(below, panel, 0.0)
    c_ref[:, here] = panel
    c_ref[here, here] = pivot_factor
    solved = nn(pivot_inverse, e_ref[here, :], exact)
    y_ref[here, :] = solved
    w_ref[...] -= nt(panel, panel, exact)
    e_ref[...] -= nn(panel, solved, exact)


def exchange_kernel(
    dims, pan_in, sum_ref, row_ref, shift_ref, pan, oth, rowbuf, sumbuf, piv, pair, wide_ref,
    panel_ref, *scratch
):
    prow, pcol, rows, cols, kept, tiles, children = dims
    (part, total, pivots, pairs, w_ref, e_ref, y_ref, c_ref, inv_ref, car_ref, g_ref,
     scale_ref, tile_ref, solved_ref, scaled_ref,
     local, part_s, part_r, sum_s, sum_r, row_s, row_r, chain_s, chain_r, cross_s, cross_r,
     oth_s, oth_r, pair_s, pair_r, gat_s, gat_r, piv_l, pair_l, load_l, store_l, scaled_l) = scratch
    del pan_in
    p, q = lax.axis_index("prow"), lax.axis_index("pcol")
    z, y = q // PANELS, lax.rem(q, PANELS)
    depth = pcol // PANELS
    home = lax.rem(q, prow)
    extent = sum_ref.shape[-1]
    band = extent // prow
    blocks = extent // STEP
    last = 2 * rows
    near = 2 * kept
    early = 4
    turns = PANELS * blocks

    barrier = pltpu.get_barrier_semaphore()
    for d in range(1, pcol):
        pl.semaphore_signal(
            barrier, inc=1, device_id={"pcol": lax.rem(q + d, pcol)}, device_id_type=MESH
        )
    for d in range(1, prow):
        pl.semaphore_signal(
            barrier, inc=1, device_id={"prow": lax.rem(p + d, prow)}, device_id_type=MESH
        )
    pl.semaphore_wait(barrier, pcol + prow - 2)

    def send(src, dst, send_sem, recv_sem, **target):
        return pltpu.make_async_remote_copy(
            src_ref=src, dst_ref=dst, send_sem=send_sem, recv_sem=recv_sem,
            device_id=target, device_id_type=MESH,
        )

    def bands(o):
        return pl.ds(pl.multiple_of(o * band, 8), band)

    def part_copy(d):
        s = lax.rem(p + d, prow)
        return send(
            sum_ref.at[0, bands(s)], part.at[d], part_s.at[d - 1], part_r.at[d - 1], prow=s
        )

    def part_own():
        return pltpu.make_async_copy(sum_ref.at[0, bands(p)], part.at[0], local.at[0])

    def sum_copy():
        d = lax.rem(home + prow - p, prow) - 1
        return send(sum_ref, sumbuf.at[d], sum_s, sum_r.at[d], prow=home)

    def sum_arrival(d):
        return send(sum_ref, sumbuf.at[d], sum_s, sum_r.at[d], prow=home)

    def reach(r):
        return sum(1 for t in range(tiles) if t * pcol < (r + 1) * prow)

    def row_copy(r, first):
        i = r * prow + p
        owner, slot = lax.rem(i, pcol), i // pcol
        window = pl.ds(first, reach(r) - first)
        return send(
            row_ref.at[r, window], rowbuf.at[slot, q, window], row_s.at[r], row_r.at[slot, q],
            pcol=owner,
        )

    def row_arrival(slot, origin, r, first):
        window = pl.ds(first, reach(r) - first)
        return send(
            row_ref.at[r, window], rowbuf.at[slot, origin, window], row_s.at[r],
            row_r.at[slot, origin], pcol=origin,
        )

    def chunk(which, n):
        if isinstance(n, int) and n == last:
            return piv.at[which, bands(p)]
        return pan.at[which, lax.div(n, 2), lax.rem(n, 2)]

    def chain_copy(n):
        ref = chunk(y, n)
        return send(ref, ref, chain_s.at[n], chain_r.at[n], pcol=q + PANELS)

    def cross_copy(n, which):
        ref = chunk(which, n)
        return send(ref, ref, cross_s.at[n], cross_r.at[n], pcol=q + 1 - 2 * y)

    def needed(n, plane):
        if isinstance(n, int) and n == last:
            return plane >= 0
        i = lax.div(n, 2) * prow + p
        used = i >= plane * PANELS
        for m, _ in PAIRS:
            used = used | (i == m)
        return used

    def step(n):
        @pl.when((z > 0) & needed(n, z))
        def _():
            chain_copy(n).wait_recv()

        @pl.when((z < depth - 1) & needed(n, z + 1))
        def _():
            chain_copy(n).start()

        @pl.when(needed(n, z))
        def _():
            cross_copy(n, y).start()

    def cross_arrival(n):
        @pl.when(needed(n, z))
        def _():
            cross_copy(n, 1 - y).wait_recv()

    def oth_row(t):
        return (t * pcol + q) // prow

    def oth_copy(t, k, d):
        n = t * PANELS + k
        return send(
            pan.at[k, oth_row(t)], oth.at[t, k], oth_s.at[n, d - 1], oth_r.at[n],
            prow=lax.rem(p + d, prow),
        )

    def pair_copy(n, d):
        m, k = PAIRS[n]
        return send(
            pan.at[k, m // prow], pair.at[n], pair_s.at[n, d - 1], pair_r.at[n],
            prow=lax.rem(p + d, prow),
        )

    def gat_copy(k, d):
        ref = piv.at[k, bands(p)]
        return send(
            ref, ref, gat_s.at[k, d - 1], gat_r.at[k, d - 1], prow=lax.rem(p + d, prow)
        )

    def gat_arrival(k, d):
        o = lax.rem(p + prow - d, prow)
        ref = piv.at[k, bands(o)]
        return send(ref, ref, gat_s.at[k, d - 1], gat_r.at[k, d - 1], prow=o)

    @pl.when(z == 0)
    def _():
        for d in range(1, prow):
            part_copy(d).start()
        part_own().start()

    for r in range(kept):
        owner = lax.rem(r * prow + p, pcol)

        @pl.when((q != owner) & (z > 0))
        def _():
            row_copy(r, 0).start()

    step(0)

    @pl.when(z == 0)
    def _():
        part_own().wait()
        for d in range(1, prow):
            part_copy(d).wait_recv()
        value = part[0]
        for d in range(1, prow):
            value = value + part[d]
        total[...] = value
        out = pltpu.make_async_copy(total, piv.at[y, bands(p)], local.at[1])
        out.start()
        out.wait()

    step(last)
    cross_arrival(last)
    for k in range(PANELS):
        for d in range(1, prow):
            gat_copy(k, d).start()

    step(1)
    step(2)
    for n in range(2):
        cross_arrival(n)
    for n, (m, k) in enumerate(PAIRS):

        @pl.when(p == m % prow)
        def _():
            for d in range(1, prow):
                pair_copy(n, d).start()

    @pl.when(p != home)
    def _():
        sum_copy().start()

    for r in range(kept):
        owner = lax.rem(r * prow + p, pcol)
        if reach(r) > 1:

            @pl.when((q != owner) & (z == 0))
            def _():
                row_copy(r, 1).start()

    step(3)
    for k in range(PANELS):
        for d in range(1, prow):
            gat_arrival(k, d).wait_recv()
    loads = [pltpu.make_async_copy(piv.at[k], pivots.at[k], piv_l.at[k]) for k in range(PANELS)]
    for load in loads:
        load.start()
    for load in loads:
        load.wait()

    def near_wait():
        for n in range(2, near):
            cross_arrival(n)

        @pl.when(p == home)
        def _():
            for t in range(cols):
                for k in range(PANELS):
                    for d in range(1, prow):
                        oth_copy(t, k, d).start()

    eye = lax.broadcasted_iota(jnp.int32, (extent, extent), 0) == lax.broadcasted_iota(
        jnp.int32, (extent, extent), 1
    )

    def joined(n, side):
        return jnp.concatenate([pairs[n, side, c] for c in range(children)], axis=1)

    @pl.loop(0, turns)
    def _(turn):
        k, block = lax.div(turn, blocks), lax.rem(turn, blocks)

        @pl.when(block == 0)
        def _():
            w_ref[...] = pivots[k] + jnp.where(eye, shift_ref[pl.ds(k, 1), :], 0.0)
            for n, (m, _) in enumerate(PAIRS):

                @pl.when(k == m)
                def _():
                    left = joined(n, 0)
                    g = g_ref[n]
                    w_ref[...] += nt(left, left) - nt(g, g)

            e_ref[...] = eye.astype(jnp.float32)

        def service():
            @pl.when(turn + early < last)
            def _():
                step(turn + early)

        factor_block(block, w_ref, e_ref, c_ref.at[k], y_ref, service)

        @pl.when(turn == turns - 3)
        def _():
            near_wait()

        @pl.when(turn == blocks - 1)
        def _():
            for n, (m, kk) in enumerate(PAIRS):

                @pl.when(p == m % prow)
                def _():
                    load = pltpu.make_async_copy(pan.at[kk, m // prow], pairs.at[n], pair_l.at[n])
                    load.start()
                    load.wait()

                @pl.when(p != m % prow)
                def _():
                    pair_copy(n, 1).wait_recv()
                    load = pltpu.make_async_copy(pair.at[n], pairs.at[n], pair_l.at[n])
                    load.start()
                    load.wait()

        @pl.when(block == blocks - 1)
        def _():
            high, low = split(y_ref[...])
            inv_ref[k, 0] = high
            inv_ref[k, 1] = low
            scale_ref[k] = jnp.sum(jnp.where(eye, c_ref[k], 0.0), axis=0, keepdims=True)

            for n, (m, kk) in enumerate(PAIRS):

                @pl.when(k == kk)
                def _():
                    right = joined(n, 1)
                    moved = split(nn(high, right) + nn(low, right))
                    left = joined(n, 0)
                    value = nt(left, moved[0]) + nt(left, moved[1])
                    for o, (mo, ko) in enumerate(PAIRS):
                        if mo == m and ko < kk:
                            slot = PAIRS.index((kk, ko))
                            for s in range(2):
                                value = value - nt(g_ref[o], car_ref[slot, s])
                    g_ref[n] = value.astype(jnp.bfloat16)

                @pl.when(k == m)
                def _():
                    g = g_ref[n]
                    one, two = split(nn(high, g) + nn(low, g))
                    car_ref[n, 0] = one
                    car_ref[n, 1] = two

    turn_at = max(rows - 2, kept)
    count = rows + cols
    left_over = max(last - early - turns, 0)
    pace = -(-left_over // rows)

    def is_row(s):
        return (s < turn_at) | (s >= turn_at + cols)

    def row_of(s):
        return jnp.where(s < turn_at, s, s - cols)

    def row_load(s):
        r = row_of(s)
        return pltpu.make_async_copy(
            pan.at[:, r], tile_ref.at[lax.rem(s, 2)], load_l.at[lax.rem(s, 2)]
        )

    def near_load(s):
        t = s - turn_at
        return pltpu.make_async_copy(
            oth.at[t], tile_ref.at[lax.rem(s, 2)], load_l.at[lax.rem(s, 2)]
        )

    def own_load(s, k):
        t = s - turn_at
        return pltpu.make_async_copy(
            pan.at[k, oth_row(t)], tile_ref.at[lax.rem(s, 2), k],
            local.at[2 + t * PANELS + k],
        )

    def begin(s):
        @pl.when(is_row(s))
        def _():
            r = row_of(s)

            @pl.when(r >= kept)
            def _():
                cross_arrival(2 * r)
                cross_arrival(2 * r + 1)

            row_load(s).start()

        @pl.when(jnp.logical_not(is_row(s)))
        def _():
            @pl.when(p == home)
            def _():
                for k in range(PANELS):
                    own_load(s, k).start()

            @pl.when(p != home)
            def _():
                for k in range(PANELS):
                    n = (s - turn_at) * PANELS + k
                    send(
                        oth.at[s - turn_at, k], oth.at[s - turn_at, k], oth_s.at[n, 0],
                        oth_r.at[n], prow=home,
                    ).wait_recv()
                near_load(s).start()

    def ready(s):
        @pl.when(is_row(s))
        def _():
            row_load(s).wait()

        @pl.when(jnp.logical_not(is_row(s)) & (p == home))
        def _():
            for k in range(PANELS):
                own_load(s, k).wait()

        @pl.when(jnp.logical_not(is_row(s)) & (p != home))
        def _():
            near_load(s).wait()

    def store(s):
        place = jnp.where(is_row(s), row_of(s), rows + s - turn_at)
        return pltpu.make_async_copy(
            solved_ref.at[lax.rem(s, 2)], wide_ref.at[place], store_l.at[lax.rem(s, 2)]
        )

    def scaled_store(s):
        return pltpu.make_async_copy(
            scaled_ref.at[lax.rem(s, 2)], panel_ref.at[row_of(s)], scaled_l.at[lax.rem(s, 2)]
        )

    begin(0)

    @pl.loop(0, count)
    def _(s):
        for c in range(pace):
            n = early + turns + pace * s + c

            @pl.when(n < last)
            def _(n=n):
                step(n)

        @pl.when(s + 1 < count)
        def _():
            begin(s + 1)

        ready(s)

        @pl.when(s >= 2)
        def _():
            store(s - 2).wait()

            @pl.when(is_row(s - 2) & (q < PANELS))
            def _():
                scaled_store(s - 2).wait()

        slot = lax.rem(s, 2)
        index = jnp.where(is_row(s), row_of(s) * prow + p, (s - turn_at) * pcol + q)
        solved = []
        for k in range(PANELS):
            left = jnp.concatenate([tile_ref[slot, k, 0, c] for c in range(children)], axis=1)
            right = jnp.concatenate([tile_ref[slot, k, 1, c] for c in range(children)], axis=1)
            moved = split(nn(inv_ref[k, 0], right) + nn(inv_ref[k, 1], right))
            value = nt(left, moved[0]) + nt(left, moved[1])
            for kk in range(k):
                pos = PAIRS.index((k, kk))
                value = value - nt(solved[kk], car_ref[pos, 0]) - nt(solved[kk], car_ref[pos, 1])
            value = jnp.where(index > k, value, 0.0)
            solved.append(value.astype(jnp.bfloat16))
            solved_ref[slot, :, k * extent : (k + 1) * extent] = solved[k]

            @pl.when((q == k) & is_row(s))
            def _(value=value, k=k):
                scaled_ref[slot] = jnp.where(index == k, c_ref[k], value) * scale_ref[k]

        store(s).start()

        @pl.when(is_row(s) & (q < PANELS))
        def _():
            scaled_store(s).start()

    for s in range(count - 2, count):
        store(s).wait()

        @pl.when(is_row(s) & (q < PANELS))
        def _():
            scaled_store(s).wait()

    for k in range(PANELS):
        for d in range(1, prow):
            gat_copy(k, d).wait_send()
    for n, (m, k) in enumerate(PAIRS):

        @pl.when(p == m % prow)
        def _():
            for d in range(1, prow):
                pair_copy(n, d).wait_send()

    @pl.when(p == home)
    def _():
        for t in range(cols):
            for k in range(PANELS):
                for d in range(1, prow):
                    oth_copy(t, k, d).wait_send()
        for d in range(prow - 1):
            sum_arrival(d).wait_recv()
        for slot in range(cols):
            for origin in range(pcol):

                @pl.when(q != origin)
                def _():
                    low = slot * pcol // prow
                    first = 1 if origin < PANELS else 0
                    if reach(low) > first:
                        row_arrival(slot, origin, low, first).wait_recv()

    @pl.when(p != home)
    def _():
        sum_copy().wait_send()

    @pl.when(z == 0)
    def _():
        for d in range(1, prow):
            part_copy(d).wait_send()

    for r in range(kept):
        owner = lax.rem(r * prow + p, pcol)

        @pl.when((q != owner) & (z > 0))
        def _():
            row_copy(r, 0).wait_send()

        if reach(r) > 1:

            @pl.when((q != owner) & (z == 0))
            def _():
                row_copy(r, 1).wait_send()

    for n in range(last + 1):

        @pl.when((z < depth - 1) & needed(n, z + 1))
        def _():
            chain_copy(n).wait_send()

        @pl.when(needed(n, z))
        def _():
            cross_copy(n, y).wait_send()


def exchange(prow, pcol, pan, sums, rowtiles, shift):
    _, rows, _, children, extent, rank = pan.shape
    cols = sums.shape[0]
    kept, tiles = rowtiles.shape[:2]
    band = extent // prow
    pairs = max(len(PAIRS), 1)
    dma = pltpu.SemaphoreType.DMA
    square = (extent, extent)
    narrow = pan.dtype
    return pl.pallas_call(
        functools.partial(exchange_kernel, (prow, pcol, rows, cols, kept, tiles, children)),
        out_shape=(
            jax.ShapeDtypeStruct(pan.shape, narrow),
            jax.ShapeDtypeStruct((cols, PANELS, 2, children, extent, rank), narrow),
            jax.ShapeDtypeStruct((cols, pcol, tiles, children, extent, rank), narrow),
            jax.ShapeDtypeStruct((prow - 1, cols) + square, jnp.float32),
            jax.ShapeDtypeStruct((PANELS,) + square, jnp.float32),
            jax.ShapeDtypeStruct((pairs, 2, children, extent, rank), narrow),
            jax.ShapeDtypeStruct((rows + cols, extent, PANELS * extent), narrow),
            jax.ShapeDtypeStruct((rows,) + square, jnp.float32),
        ),
        in_specs=[ANY, ANY, ANY, pl.BlockSpec(memory_space=pltpu.VMEM)],
        out_specs=(ANY,) * 8,
        scratch_shapes=[
            pltpu.VMEM((prow, band, extent), jnp.float32),
            pltpu.VMEM((band, extent), jnp.float32),
            pltpu.VMEM((PANELS,) + square, jnp.float32),
            pltpu.VMEM((pairs, 2, children, extent, rank), narrow),
            pltpu.VMEM(square, jnp.float32),
            pltpu.VMEM(square, jnp.float32),
            pltpu.VMEM(square, jnp.float32),
            pltpu.VMEM((PANELS,) + square, jnp.float32),
            pltpu.VMEM((PANELS, 2) + square, narrow),
            pltpu.VMEM((pairs, 2) + square, narrow),
            pltpu.VMEM((pairs,) + square, narrow),
            pltpu.VMEM((PANELS, 1, extent), jnp.float32),
            pltpu.VMEM((2, PANELS, 2, children, extent, rank), narrow),
            pltpu.VMEM((2, extent, PANELS * extent), narrow),
            pltpu.VMEM((2,) + square, jnp.float32),
            dma((2 + cols * PANELS,)),
            dma((prow - 1,)),
            dma((prow - 1,)),
            dma,
            dma((prow - 1,)),
            dma((kept,)),
            dma((cols, pcol)),
            dma((2 * rows + 1,)),
            dma((2 * rows + 1,)),
            dma((2 * rows + 1,)),
            dma((2 * rows + 1,)),
            dma((cols * PANELS, prow - 1)),
            dma((cols * PANELS,)),
            dma((pairs, prow - 1)),
            dma((pairs,)),
            dma((PANELS, prow - 1)),
            dma((PANELS, prow - 1)),
            dma((PANELS,)),
            dma((pairs,)),
            dma((2,)),
            dma((2,)),
            dma((2,)),
        ],
        input_output_aliases={0: 0},
        compiler_params=pltpu.CompilerParams(
            collective_id=0, has_side_effects=True, vmem_limit_bytes=67_043_328
        ),
        cost_estimate=pl.CostEstimate(
            flops=120_000_000_000, bytes_accessed=90 * 2**20, transcendentals=0
        ),
        name="exchange",
    )(pan, sums, rowtiles, shift)


def diag_kernel(dims, at_ref, rowbuf, pan_ref, own_ref, sums_ref, mine_ref, shift_ref, d_ref):
    prow, pcol, kept = dims
    slot = pl.program_id(0)
    tiles, children, extent = rowbuf.shape[2], rowbuf.shape[3], rowbuf.shape[4]
    q = at_ref[1]

    @pl.when(at_ref[0] == lax.rem(q, prow))
    def _():
        eye = lax.broadcasted_iota(jnp.int32, (extent, extent), 0) == lax.broadcasted_iota(
            jnp.int32, (extent, extent), 1
        )
        shift = shift_ref[pl.ds(slot * pcol + q, 1), :]
        total = mine_ref[0] + jnp.where(eye, shift, 0.0)
        for s in range(sums_ref.shape[0]):
            total = total + sums_ref[s, 0]
        for t in range(tiles):
            own = jnp.concatenate([own_ref[0, t, c] for c in range(children)], axis=1)
            if t > 0:
                total = total + nt(own, own)
            else:
                total = total + jnp.where(q >= PANELS, nt(own, own), 0.0)
        for k in range(PANELS):
            tile = jnp.concatenate([pan_ref[k, 0, 0, c] for c in range(children)], axis=1)
            total = total + nt(tile, tile)
        d_ref[0] = total
        for origin in range(pcol):
            for t in range(tiles):
                if t == 0 and origin < PANELS:
                    continue

                @pl.when((q != origin) & (t * pcol < slot * pcol + q))
                def _():
                    tile = jnp.concatenate(
                        [rowbuf[0, origin, t, c] for c in range(children)], axis=1
                    )
                    d_ref[0] += nt(tile, tile)


def diag(prow, pcol, at, rowbuf, pan, rowtiles, sumbuf, sums, shift):
    cols, _, tiles, children, extent, rank = rowbuf.shape
    kept = rowtiles.shape[0]
    others = sumbuf.shape[0]

    def row(slot, at):
        return (slot * pcol + at[1]) // prow

    return pl.pallas_call(
        functools.partial(diag_kernel, (prow, pcol, kept)),
        out_shape=jax.ShapeDtypeStruct((cols, extent, extent), jnp.float32),
        grid_spec=pltpu.PrefetchScalarGridSpec(
            num_scalar_prefetch=1,
            grid=(cols,),
            in_specs=[
                pl.BlockSpec(
                    (1, pcol, tiles, children, extent, rank), lambda s, at: (s, 0, 0, 0, 0, 0)
                ),
                pl.BlockSpec(
                    (PANELS, 1, 1, children, extent, rank),
                    lambda s, at: (0, row(s, at), 0, 0, 0, 0),
                ),
                pl.BlockSpec(
                    (1, tiles, children, extent, rank), lambda s, at: (row(s, at), 0, 0, 0, 0)
                ),
                pl.BlockSpec((others, 1, extent, extent), lambda s, at: (0, s, 0, 0)),
                pl.BlockSpec((1, extent, extent), lambda s, at: (s, 0, 0)),
                pl.BlockSpec(shift.shape, lambda s, at: (0, 0)),
            ],
            out_specs=pl.BlockSpec((1, extent, extent), lambda s, at: (s, 0, 0)),
        ),
        compiler_params=pltpu.CompilerParams(vmem_limit_bytes=67_043_328),
        cost_estimate=pl.CostEstimate(
            flops=6_000_000_000, bytes_accessed=24 * 2**20, transcendentals=0
        ),
        name="diag",
    )(at, rowbuf, pan, rowtiles, sumbuf, sums, shift)


def finish_kernel(dims, at_ref, rank_ref, u_ref, v_ref, g_ref, h_ref, d_ref, p_ref, o_ref):
    prow, pcol = dims
    r = pl.program_id(0)
    children, cols = u_ref.shape[0], u_ref.shape[3]
    extent, rank_max = u_ref.shape[-2:]
    pieces = extent // STEP
    lane = lax.broadcasted_iota(jnp.int32, (1, rank_max), 1)
    i = r * prow + at_ref[0]

    for t in range(cols):
        j = t * pcol + at_ref[1]

        def put(value, t=t):
            for s in range(pieces):
                o_ref[pl.ds(t * pieces + s, extent, stride=cols * pieces), :] = value[
                    :, s * STEP : (s + 1) * STEP
                ]

        @pl.when(i < j)
        def _():
            put(jnp.zeros((extent, extent), jnp.float32))

        if t == 0:

            @pl.when((i >= j) & (j < PANELS))
            def _():
                put(p_ref[0])

        def total(t=t):
            left, right = [], []
            for c in range(children):
                rank = rank_ref[(c * pl.num_programs(0) + r) * cols + t]
                keep = (lane < rank).astype(jnp.bfloat16)
                left.append(u_ref[c, 0, 0, t, 0])
                right.append(v_ref[c, 0, 0, t, 0] * keep)
            value = nt(jnp.concatenate(left, axis=1), jnp.concatenate(right, axis=1))
            return value - nt(g_ref[0], h_ref[t])

        @pl.when((i > j) & (j >= PANELS))
        def _():
            put(total())

        @pl.when((i == j) & (j >= PANELS))
        def _():
            put(total() + d_ref[t])


def finish(prow, pcol, at, ranks, child_u, child_v, wide, diags, panels):
    children, rows, _, cols, _, extent, rank = child_u.shape
    width = wide.shape[-1]
    lines = extent * cols * extent // STEP
    tile = pl.BlockSpec(
        (children, 1, 1, cols, 1, extent, rank), lambda r, at, ranks: (0, r, 0, 0, 0, 0, 0)
    )
    return pl.pallas_call(
        functools.partial(finish_kernel, (prow, pcol)),
        out_shape=jax.ShapeDtypeStruct((rows * lines, STEP), jnp.float32),
        grid_spec=pltpu.PrefetchScalarGridSpec(
            num_scalar_prefetch=2,
            grid=(rows,),
            in_specs=[
                tile,
                tile,
                pl.BlockSpec((1, extent, width), lambda r, at, ranks: (r, 0, 0)),
                pl.BlockSpec((cols, extent, width), lambda r, at, ranks: (rows // cols, 0, 0)),
                pl.BlockSpec((cols, extent, extent), lambda r, at, ranks: (0, 0, 0)),
                pl.BlockSpec(
                    (1, extent, extent),
                    lambda r, at, ranks: (jnp.where(at[1] < PANELS, r, 0), 0, 0),
                ),
            ],
            out_specs=pl.BlockSpec((lines, STEP), lambda r, at, ranks: (r, 0)),
        ),
        compiler_params=pltpu.CompilerParams(vmem_limit_bytes=67_043_328),
        cost_estimate=pl.CostEstimate(
            flops=2 * rows * cols * extent * extent * (width + children * rank),
            bytes_accessed=50 * 2**20,
            transcendentals=0,
        ),
        name="finish",
    )(at, ranks, child_u, child_v, wide, wide, diags, panels)


def on_device(prow, pcol, child_u, child_v, child_rank, diag_shift):
    own_row, own_column = lax.axis_index("prow"), lax.axis_index("pcol")
    children, rows, _, cols, _, extent, rank = child_u.shape
    kept = cols * pcol // prow
    tiles = cols
    at = jnp.stack([own_row, own_column]).astype(jnp.int32)
    ranks = child_rank.reshape(-1)
    pan, sums, rowtiles = prep(prow, pcol, kept, tiles, at, ranks, child_u, child_v)
    pan, _, rowbuf, sumbuf, _, _, wide, panels = exchange(
        prow, pcol, pan, sums, rowtiles, diag_shift
    )
    diags = diag(prow, pcol, at, rowbuf, pan, rowtiles, sumbuf, sums, diag_shift)
    out = finish(prow, pcol, at, ranks, child_u, child_v, wide, diags, panels)
    return out.reshape(rows, 1, extent, cols, 1, extent)


def solution(mesh):
    placed = (
        P(None, None, "prow", None, "pcol", None, None),
        P(None, None, "prow", None, "pcol", None, None),
        P(None, None, "prow", None, "pcol"),
        P(),
    )
    return jax.shard_map(
        functools.partial(on_device, mesh.shape["prow"], mesh.shape["pcol"]),
        mesh=mesh,
        in_specs=placed,
        out_specs=P(None, "prow", None, None, "pcol", None),
        check_vma=False,
    )
```
